32 devices in a mesh: tilt: 2 (over y), row: 8 (over z, x), col: 2 (over core).
Axes of the slice: x: 2, y: 2, z: 4, core: 2. Of those that a mesh axis runs over, the one named last changes fastest.
Arguments:
- object_field: float32 [2, 2048, 256], P(None, ('tilt', 'row'), 'col'), parts along dimension 1, may hold values from -4.2 to 4.2
- probe: float32 [8, 2, 128, 128], P('tilt'), parts along dimension 0, may hold values from -2.1 to 2.1
- patterns: float32 [16, 2, 2, 128, 128], P(('tilt', 'row'), 'col'), parts along dimension 0, may hold values from 0.1 to 3
- offsets: int32 [16, 2, 2, 2], P(('tilt', 'row'), 'col'), parts along dimension 0, may hold values from 0 to 256
- counts: int32 [16, 2], P(('tilt', 'row'), 'col'), parts along dimension 0, may hold values from 1 to 2, as said below
Outputs:
- object_out: float32 [2, 2048, 256], P(None, ('tilt', 'row'), 'col'), parts along dimension 1
- probe_out: float32 [8, 2, 128, 128], P('tilt'), parts along dimension 0
The draws below stay inside these ranges and needn't reach their ends.
There are 2 independent parts, one for each index of `tilt`. The reference program is written for one: setup_inputs(seed, part) draws one part's arguments, and reference() takes and returns one part's arrays. A program takes and returns all parts, laid end to end along the dimension named above; each array names one. Nothing has to cross between parts.
Inputs may be any that keep to these rules, and one draw needn't show every extreme that they name: Only the first counts[r, c] slots of a tile are live; some tile has all 2 live. `offsets`: A window lies inside its tile's frame of 384 pixels a side.
All inputs are finite; a program needn't handle non-finite values.
Results may differ from the reference program's by a relative error of at most 0.0003.
Values sent between devices are 32-bit elements; how exact they have to be, the bound alone decides.
A program may use at most 64 MiB of HBM per device.

```python
import math
import jax
import jax.numpy as jnp
from jax import lax

B = 128
H = 128
P_SIZE = 128
MODES = 4
POS = 2
ITERS = 1
TILE_ROWS = 8
TILE_COLS = 2
NY = 1024
NX = 256


def draw_counts(key, part):
    light_key = jax.random.fold_in(key, 101)
    busy_key = jax.random.fold_in(key, 202)
    chosen_key = jax.random.fold_in(key, 303)
    light_tiles = jax.random.randint(light_key, (TILE_ROWS, TILE_COLS), 1, max(POS // 2, 1) + 1)
    busy_tiles = jax.random.randint(busy_key, (TILE_ROWS, TILE_COLS), 0, 8) == 0
    filled = jnp.where(busy_tiles, POS, light_tiles).reshape(-1)
    chosen_tile = jax.random.randint(chosen_key, (), 0, TILE_ROWS * TILE_COLS)
    filled = filled.at[chosen_tile].set(POS)
    return filled.reshape(TILE_ROWS, TILE_COLS).astype(jnp.int32)


def plant(result, rng, least, top_value):
    shape = result.shape
    spot = [jax.random.randint(jax.random.fold_in(rng, axis), (), 0, shape[axis]) for axis in range(len(shape))]
    result = result.at[tuple(spot)].set(least)
    longest = shape.index(max(shape))
    spot[longest] = (spot[longest] + 1) % shape[longest]
    return result.at[tuple(spot)].set(top_value)


def steps_of(rng, shape, shards, least, top_value):
    def one(dim, blocks):
        draws = jax.random.uniform(jax.random.fold_in(jax.random.fold_in(rng, 6), dim), (blocks,), jnp.float32, least / len(shards), top_value / len(shards))
        return jnp.repeat(jnp.exp(draws), shape[dim] // blocks).reshape((-1,) + (1,) * (len(shape) - dim - 1))

    factor_of = one(*shards[0])
    for cut in shards[1:]:
        factor_of = factor_of * one(*cut)
    return factor_of


def scatter_about(key, dims, spread, most, cuts=(), kind=jnp.bfloat16):
    entries = spread * jax.random.normal(key, dims, jnp.float32)
    if cuts:
        entries = entries * steps_of(key, dims, cuts, -0.22, 0.18)
    return jnp.clip(entries, -most, most).astype(kind)


def setup_inputs(seed: int = 0, part: int = 0) -> dict:
    keys = jax.random.split(jax.random.key(seed), 6)
    part_keys = jax.random.split(jax.random.fold_in(keys[5], part), 6)
    object_field = scatter_about(part_keys[0], (2, NY, NX), 0.7, 4.2, ((1, 8), (2, 2)), jnp.float32)
    probe = scatter_about(part_keys[1], (MODES, 2, P_SIZE, P_SIZE), 0.35, 2.1, (), jnp.float32)
    patterns = jnp.clip(jnp.exp(math.log(3.0) - 3.4011974 * jax.random.uniform(part_keys[2], (TILE_ROWS, TILE_COLS, POS, P_SIZE, P_SIZE), jnp.float32) ** steps_of(part_keys[2], (TILE_ROWS, TILE_COLS, POS, P_SIZE, P_SIZE), ((0, 8), (1, 2)), -0.2, 0.2)), 0.1, 3.0)
    offsets = plant(jax.random.randint(part_keys[3], (TILE_ROWS, TILE_COLS, POS, 2), 0, B + 2 * H - P_SIZE + 1), jax.random.fold_in(part_keys[3], 1), 0, B + 2 * H - P_SIZE).astype(jnp.int32)
    counts = draw_counts(jax.random.fold_in(jax.random.fold_in(keys[5], part), 71), part)
    return dict(object_field=object_field, probe=probe, patterns=patterns, offsets=offsets, counts=counts)


object_rate = 1.0
probe_rate = 1.0
epsilon = 1e-06

def as_index(value):
    return jnp.asarray(value).astype(jnp.int32)

def dft_tables(length):
    counter = jnp.arange(length, dtype=jnp.int32)
    product = counter[:, None] * counter[None, :] % length
    angle = -2.0 * jnp.pi / length * product.astype(jnp.float32)
    norm = 1.0 / jnp.sqrt(jnp.float32(length))
    return (jnp.cos(angle) * norm, jnp.sin(angle) * norm)

def left_product(cos_table, sin_table, real_part, imag_part):
    hp = lax.Precision.HIGHEST
    real_out = jnp.einsum('ab,kbc->kac', cos_table, real_part, precision=hp) - jnp.einsum('ab,kbc->kac', sin_table, imag_part, precision=hp)
    imag_out = jnp.einsum('ab,kbc->kac', cos_table, imag_part, precision=hp) + jnp.einsum('ab,kbc->kac', sin_table, real_part, precision=hp)
    return (real_out, imag_out)

def right_product(real_part, imag_part, cos_table, sin_table):
    hp = lax.Precision.HIGHEST
    real_out = jnp.einsum('kab,bc->kac', real_part, cos_table, precision=hp) - jnp.einsum('kab,bc->kac', imag_part, sin_table, precision=hp)
    imag_out = jnp.einsum('kab,bc->kac', real_part, sin_table, precision=hp) + jnp.einsum('kab,bc->kac', imag_part, cos_table, precision=hp)
    return (real_out, imag_out)

def transform(real_part, imag_part, cos_table, sin_table):
    middle_re, middle_im = left_product(cos_table, sin_table, real_part, imag_part)
    return right_product(middle_re, middle_im, cos_table, sin_table)

def slot_terms(window, probe, pattern, cos_table, sin_table):
    window_re, window_im = (window[0], window[1])
    probe_re, probe_im = (probe[:, 0], probe[:, 1])
    exit_re = probe_re * window_re - probe_im * window_im
    exit_im = probe_re * window_im + probe_im * window_re
    far_re, far_im = transform(exit_re, exit_im, cos_table, sin_table)
    intensity = lax.optimization_barrier(jnp.sum(far_re * far_re + far_im * far_im, axis=0))
    misfit = intensity - pattern
    back_re, back_im = transform(misfit * far_re, misfit * far_im, cos_table, -sin_table)
    grad_re = lax.optimization_barrier(jnp.sum(probe_re * back_re + probe_im * back_im, axis=0))
    grad_im = lax.optimization_barrier(jnp.sum(probe_re * back_im - probe_im * back_re, axis=0))
    term_re = window_re * back_re + window_im * back_im
    term_im = window_re * back_im - window_im * back_re
    return (jnp.stack([grad_re, grad_im]), jnp.stack([term_re, term_im], axis=1))

def reference(object_field, probe, patterns, offsets, counts):
    cos_table, sin_table = dft_tables(P_SIZE)
    frame_size = B + 2 * H
    for iteration in range(ITERS):
        padded = jnp.pad(object_field, ((0, 0), (H, H), (H, H)))

        def tile_step(carry, tile_index):
            gradient, probe_grad = carry
            tile_row = as_index(tile_index // TILE_COLS)
            tile_col = as_index(tile_index % TILE_COLS)
            frame = lax.dynamic_slice(padded, (as_index(0), tile_row * B, tile_col * B), (2, frame_size, frame_size))

            def slot_step(slot_index, inner):
                local_grad, probe_acc = inner
                slot_index = as_index(slot_index)
                corner_y = as_index(offsets[tile_row, tile_col, slot_index, 0])
                corner_x = as_index(offsets[tile_row, tile_col, slot_index, 1])
                window = lax.dynamic_slice(frame, (as_index(0), corner_y, corner_x), (2, P_SIZE, P_SIZE))
                window_grad, probe_term = slot_terms(window, probe, patterns[tile_row, tile_col, slot_index], cos_table, sin_table)
                live = (slot_index < counts[tile_row, tile_col]).astype(jnp.float32)
                region = lax.dynamic_slice(local_grad, (as_index(0), corner_y, corner_x), (2, P_SIZE, P_SIZE)) + live * window_grad
                local_grad = lax.dynamic_update_slice(local_grad, region, (as_index(0), corner_y, corner_x))
                return (local_grad, probe_acc + live * probe_term)
            local_grad = jnp.zeros((2, frame_size, frame_size), jnp.float32)
            local_grad, probe_grad = lax.fori_loop(0, POS, slot_step, (local_grad, probe_grad))
            start = (as_index(0), tile_row * B, tile_col * B)
            region = lax.dynamic_slice(gradient, start, (2, frame_size, frame_size)) + local_grad
            gradient = lax.dynamic_update_slice(gradient, region, start)
            return ((gradient, probe_grad), None)
        start_carry = (jnp.zeros_like(padded), jnp.zeros_like(probe))
        (gradient, probe_grad), unused = lax.scan(tile_step, start_carry, jnp.arange(TILE_ROWS * TILE_COLS, dtype=jnp.int32))
        object_grad = gradient[:, H:H + NY, H:H + NX]
        weight = jnp.max(lax.optimization_barrier(jnp.sum(probe[:, 0] * probe[:, 0] + probe[:, 1] * probe[:, 1], axis=0))) + epsilon
        object_field = object_field - object_rate * object_grad / weight
        probe = probe - probe_rate * probe_grad / (TILE_ROWS * TILE_COLS)
    return (object_field, probe)
```

```python
import contextlib
import functools

import jax
import jax.numpy as jnp
import numpy as np
from jax import lax
from jax.experimental import pallas as pl
from jax.experimental.pallas import tpu as pltpu
from jax.sharding import PartitionSpec as P

MESH = pl.DeviceIdType.MESH
F32 = jnp.float32
BF16 = jnp.bfloat16

object_rate = 1.0
probe_rate = 1.0
epsilon = 1e-06


def mark(name):
    return contextlib.nullcontext()


def split_table(table):
    high = table.astype(jnp.bfloat16)
    low = (table - high.astype(np.float64)).astype(jnp.bfloat16)
    return high, low


def dft_tables(length):
    counter = np.arange(length)
    product = counter[:, None] * counter[None, :] % length
    angle = -2.0 * np.pi / length * product
    c, s = np.cos(angle) / np.sqrt(length), np.sin(angle) / np.sqrt(length)
    right = np.block([[c, s], [-s, c]])
    left = right.T
    return np.stack([*split_table(right), *split_table(left)])


def split(x):
    high = x.astype(BF16)
    return high, (x - high.astype(F32)).astype(BF16)


def dot(a, b):
    return jnp.dot(a, b, preferred_element_type=F32)


def plan(rows):
    assert rows & (rows - 1) == 0
    group = min(4, rows)
    ways = []
    while group << len(ways) < rows:
        ways.append(group << len(ways))
    return group, ways


CUTS = 2
STRIPS = 2


def kernel(
    rows, modes, slots, width,
    off_hbm, cnt_hbm, obj_hbm, probe_hbm, pat_hbm, tab_hbm,
    obj_out, probe_out,
    off_ref, cnt_ref, probe_ref, pat_ref, tab_ref,
    frame, xh, xl, yh, yl, far, vh, vl, win, gacc,
    gown, gpar, grecv, gedge, term, tpart, acc, pieces, part, swapped, fin, fin_other,
    load, hm_send, hm_recv, h_send, h_recv, r_send, r_recv, g_send, g_recv, e_send, e_recv, t_send, t_recv,
    rs_send, rs_recv, x_send, x_recv, ag_send, ag_recv, o_send, o_recv,
):
    me = lax.axis_index("row")
    col = lax.axis_index("col")
    n = width
    tiles = rows * 2
    pairs = modes // 2
    group, ways = plan(rows)
    slab = 2 * n // group
    chunk = slab // CUTS
    mate = {"col": 1 - col}
    up = {"row": me - 1}
    down = {"row": me + 1}
    has_up, has_down = me > 0, me < rows - 1
    seat = lax.rem(me, group)

    def flip(index, bit):
        return jnp.where(lax.rem(index // bit, 2) == 0, index + bit, index - bit)

    def hop_to(index, hop):
        for b in range(hop.bit_length()):
            if hop >> b & 1:
                index = flip(index, 1 << b)
        return index

    def mode_at(spot):
        return 2 * spot + 1 - col if spot < pairs else 2 * (spot - pairs) + col

    loads = [
        pltpu.make_async_copy(obj_hbm, frame.at[1, 1], load.at[0]),
        pltpu.make_async_copy(off_hbm, off_ref, load.at[1]),
        pltpu.make_async_copy(cnt_hbm, cnt_ref, load.at[2]),
        pltpu.make_async_copy(pat_hbm, pat_ref, load.at[3]),
        pltpu.make_async_copy(tab_hbm, tab_ref, load.at[4]),
    ]
    probes = [
        pltpu.make_async_copy(probe_hbm.at[mode_at(j)], probe_ref.at[j], load.at[5 + j]) for j in range(modes)
    ]

    barrier = pltpu.get_barrier_semaphore()

    def greet(to):
        pl.semaphore_signal(barrier, inc=1, device_id=to, device_id_type=MESH)

    pl.when(has_up)(lambda: greet(up))
    pl.when(has_down)(lambda: greet(down))
    for hop in range(1, group):
        greet({"row": hop_to(me, hop)})
    for way in ways:
        greet({"row": flip(me, way)})
    greet(mate)
    for copy in loads + probes:
        copy.start()
    with mark("w_barrier"):
        pl.semaphore_wait(
            barrier, 1 + has_up.astype(jnp.int32) + has_down.astype(jnp.int32) + group - 1 + len(ways)
        )

    def remote(src, dst, send, recv, to):
        return pltpu.make_async_remote_copy(
            src_ref=src, dst_ref=dst, send_sem=send, recv_sem=recv, device_id=to, device_id_type=MESH
        )

    seen = 2 * col
    mine = 2 - 2 * col
    strip = n // STRIPS
    strips = [(q, pl.ds(h * strip, strip)) for q in range(2) for h in range(STRIPS)]
    to_mate = remote(obj_hbm, frame.at[1, seen], hm_send.at[0], hm_recv.at[0], mate)

    def halo(side, i):
        q, at = strips[i]
        return remote(
            obj_hbm.at[q, at], frame.at[2 * side, 1, q, at], h_send.at[side, i], h_recv.at[side, i], (down, up)[side]
        )

    def relay(side, i):
        q, at = strips[i]
        return remote(
            frame.at[2 * side, 1, q, at], frame.at[2 * side, seen, q, at],
            r_send.at[side, i], r_recv.at[side, i], mate,
        )

    sent = ((0, has_down), (1, has_up))
    got = ((0, has_up), (1, has_down))

    @pl.when(lax.rem(me, 2) == 0)
    def _():
        for side, has in sent[::-1]:
            for i in range(len(strips)):
                pl.when(has)(halo(side, i).start)

    @pl.when(lax.rem(me, 2) == 1)
    def _():
        for side, has in sent:
            for i in range(len(strips)):
                pl.when(has)(halo(side, i).start)

    to_mate.start()

    zero = jnp.zeros((2, n, n), F32)
    for j in range(3):
        frame[j, seen] = zero

    @pl.when(me == 0)
    def _():
        frame[0, 1] = zero
        frame[0, mine] = zero
        gedge[0] = zero

    @pl.when(me == rows - 1)
    def _():
        frame[2, 1] = zero
        frame[2, mine] = zero
        gedge[1] = zero

    with mark("w_load"):
        for copy in probes:
            copy.wait()
    power = jnp.zeros((n, n), F32)
    for k in range(modes):
        power = power + (probe_ref[k, 0] * probe_ref[k, 0] + probe_ref[k, 1] * probe_ref[k, 1])
    weight = jnp.max(power) + epsilon

    with mark("w_halo"):
        @pl.when(lax.rem(me, 2) == 0)
        def _():
            for side, has in got[::-1]:
                for i in range(len(strips)):
                    @pl.when(has)
                    def _():
                        halo(side, i).wait_recv()
                        relay(side, i).start()

        @pl.when(lax.rem(me, 2) == 1)
        def _():
            for side, has in got:
                for i in range(len(strips)):
                    @pl.when(has)
                    def _():
                        halo(side, i).wait_recv()
                        relay(side, i).start()

    for copy in loads:
        copy.wait()
    to_mate.wait_recv()
    with mark("w_relay"):
        for side, has in got:
            for i in range(len(strips)):
                pl.when(has)(relay(side, i).wait_recv)

    r_hi, r_lo, l_hi, l_lo = (tab_ref.at[t] for t in range(4))
    row_id = lax.broadcasted_iota(jnp.int32, (n, n), 0)
    lane_id = lax.broadcasted_iota(jnp.int32, (n, n), 1)

    def place(s):
        oy, ox = off_ref[0, 0, s, 0], off_ref[0, 0, s, 1]
        by, bx = oy // n, ox // n
        return by, bx, oy - by * n, ox - bx * n

    for s in range(slots):
        by, bx, sy, sx = place(s)
        by2, bx2 = jnp.minimum(by + 1, 2), jnp.minimum(bx + 1, 2)
        for q in range(2):
            upper = jnp.where(lane_id >= sx, frame[by, bx, q], frame[by, bx2, q])
            lower = jnp.where(lane_id >= sx, frame[by2, bx, q], frame[by2, bx2, q])
            packed = jnp.where(row_id >= sy, upper, lower)
            packed = pltpu.roll(packed, lax.rem(n - sy, n), 0)
            win[s, q] = pltpu.roll(packed, lax.rem(n - sx, n), 1)
        for k in range(modes):
            wr, wi = win[s, 0], win[s, 1]
            pr, pi = probe_ref[k, 0], probe_ref[k, 1]
            for q, value in enumerate((pr * wr - pi * wi, pr * wi + pi * wr)):
                hi, lo = split(value)
                xh[s, k * n : (k + 1) * n, q * n : (q + 1) * n] = hi
                xl[s, k * n : (k + 1) * n, q * n : (q + 1) * n] = lo
        for k in range(modes):
            a_hi, a_lo = xh[s, k * n : (k + 1) * n, :], xl[s, k * n : (k + 1) * n, :]
            y = dot(a_hi, r_hi[...]) + dot(a_lo, r_hi[...]) + dot(a_hi, r_lo[...])
            for q in range(2):
                hi, lo = split(y[:, q * n : (q + 1) * n])
                yh[s, q * n : (q + 1) * n, k * n : (k + 1) * n] = hi
                yl[s, q * n : (q + 1) * n, k * n : (k + 1) * n] = lo
        for p in range(modes // 2):
            cols = slice(2 * p * n, 2 * (p + 1) * n)
            b_hi, b_lo = yh[s, :, cols], yl[s, :, cols]
            far[s, :, cols] = dot(l_hi[...], b_hi) + dot(l_lo[...], b_hi) + dot(l_hi[...], b_lo)
        level = jnp.zeros((n, n), F32)
        for k in range(modes):
            cols = slice(k * n, (k + 1) * n)
            level = level + far[s, :n, cols] * far[s, :n, cols] + far[s, n:, cols] * far[s, n:, cols]
        live = (s < cnt_ref[0, 0]).astype(F32)
        misfit = live * (level - pat_ref[0, 0, s])
        for k in range(modes):
            for q in range(2):
                spot = (s, slice(q * n, (q + 1) * n), slice(k * n, (k + 1) * n))
                hi, lo = split(misfit * far[spot])
                yh[spot] = hi
                yl[spot] = lo

    def to_partner(p):
        return remote(term.at[p], tpart.at[p], t_send.at[p], t_recv.at[p], mate)

    def rows_of(owner, c):
        return pl.ds(pl.multiple_of(owner * slab + c * chunk, 8), chunk)

    def scatter(p, c, hop):
        return remote(
            acc.at[p, rows_of(hop_to(seat, hop), c)], pieces.at[hop - 1, p, pl.ds(c * chunk, chunk)],
            rs_send.at[hop - 1, p, c], rs_recv.at[hop - 1, p, c], {"row": hop_to(me, hop)},
        )

    hops = list(range(1, group))
    for b in range(modes // 2):
        cols = slice(2 * b * n, 2 * (b + 1) * n)
        for s in range(slots):
            b_hi, b_lo = yh[s, :, cols], yl[s, :, cols]
            v = dot(r_hi[...], b_hi) + dot(r_lo[...], b_hi) + dot(r_hi[...], b_lo)
            for m in range(2):
                for q in range(2):
                    hi, lo = split(v[q * n : (q + 1) * n, m * n : (m + 1) * n])
                    vh[s, m * n : (m + 1) * n, q * n : (q + 1) * n] = hi
                    vl[s, m * n : (m + 1) * n, q * n : (q + 1) * n] = lo
        for m in range(2):
            k = 2 * b + m
            for s in range(slots):
                a_hi, a_lo = vh[s, m * n : (m + 1) * n, :], vl[s, m * n : (m + 1) * n, :]
                back = dot(a_hi, l_hi[...]) + dot(a_lo, l_hi[...]) + dot(a_hi, l_lo[...])
                br, bi = back[:, :n], back[:, n:]
                pr, pi = probe_ref[k, 0], probe_ref[k, 1]
                gr, gi = pr * br + pi * bi, pr * bi - pi * br
                wr, wi = win[s, 0], win[s, 1]
                tr, ti = wr * br + wi * bi, wr * bi - wi * br
                if k == 0:
                    gacc[s, 0], gacc[s, 1] = gr, gi
                else:
                    gacc[s, 0], gacc[s, 1] = gacc[s, 0] + gr, gacc[s, 1] + gi
                if s == 0:
                    term[k, :n], term[k, n:] = tr, ti
                else:
                    term[k, :n], term[k, n:] = term[k, :n] + tr, term[k, n:] + ti
            if k < pairs:
                to_partner(k).start()
            else:
                p = k - pairs
                with mark("w_partner"):
                    to_partner(p).wait_recv()
                acc[p] = term[k] + tpart[p]
                for c in range(CUTS):
                    for hop in hops:
                        scatter(p, c, hop).start()

    def across(j):
        return remote(gpar.at[j], grecv.at[j], g_send.at[j], g_recv.at[j], mate)

    for q in range(2):
        own = [jnp.zeros((n, n), F32)] * 3
        par = [jnp.zeros((n, n), F32)] * 3
        for s in range(slots):
            by, bx, sy, sx = place(s)
            g = pltpu.roll(pltpu.roll(gacc[s, q], sy, 0), sx, 1)
            low_x, low_y = (lane_id >= sx).astype(F32), (row_id >= sy).astype(F32)

            def side_of(block, at, low):
                return (block == at).astype(F32) * low + (block == at + 1).astype(F32) * (1.0 - low)

            g_own, g_par = g * side_of(1, bx, low_x), g * side_of(mine, bx, low_x)
            for j in range(3):
                mask = side_of(j, by, low_y)
                own[j] = own[j] + g_own * mask
                par[j] = par[j] + g_par * mask
        for j in range(3):
            gown[j, q] = own[j]
            gpar[j, q] = par[j]
    for j in (0, 2, 1):
        across(j).start()

    edge_up = remote(gown.at[0], gedge.at[1], e_send.at[0], e_recv.at[1], up)
    edge_down = remote(gown.at[2], gedge.at[0], e_send.at[1], e_recv.at[0], down)
    with mark("w_across"):
        for j, has, edge in ((0, has_up, edge_up), (2, has_down, edge_down)):
            across(j).wait_recv()
            gown[j] = gown[j] + grecv[j]
            pl.when(has)(edge.start)

    chunks = [(p, c) for p in range(pairs) for c in range(CUTS)]

    def exchange(r, p, c):
        at = pl.ds(c * chunk, chunk)
        return remote(
            part.at[r, p, at], swapped.at[r, p, at], x_send.at[r, p, c], x_recv.at[r, p, c],
            {"row": flip(me, ways[r])},
        )

    def gather(p, c, hop):
        here = fin.at[p, rows_of(seat, c)]
        return remote(
            here, here, ag_send.at[hop - 1, p, c], ag_recv.at[hop - 1, p, c], {"row": hop_to(me, hop)}
        )

    def share(p, c, hop):
        at = rows_of(hop_to(seat, hop), c)
        return remote(fin.at[p, at], fin_other.at[p, at], o_send.at[hop, p, c], o_recv.at[hop, p, c], mate)

    def settle(r, p, c, total):
        if r < len(ways):
            part[r, p, c * chunk : (c + 1) * chunk] = total
            exchange(r, p, c).start()
        else:
            fin[p, rows_of(seat, c)] = total
            for hop in hops:
                gather(p, c, hop).start()
            share(p, c, 0).start()

    for p, c in chunks:
        total = acc[p, rows_of(seat, c)]
        with mark("w_rs"):
            for hop in hops:
                scatter(p, c, hop).wait_recv()
        for hop in hops:
            total = total + pieces[hop - 1, p, c * chunk : (c + 1) * chunk]
        settle(0, p, c, total)
    for r in range(len(ways)):
        for p, c in chunks:
            with mark("w_xc"):
                exchange(r, p, c).wait_recv()
            at = slice(c * chunk, (c + 1) * chunk)
            settle(r + 1, p, c, part[r, p, at] + swapped[r, p, at])

    with mark("w_edge"):
        across(1).wait_recv()
        pl.when(has_up)(edge_down.wait_recv)
        pl.when(has_down)(edge_up.wait_recv)
    for q in range(2):
        grad = gown[1, q] + grecv[1, q] + gedge[0, q] + gedge[1, q]
        obj_out[q] = frame[1, 1, q] - object_rate * grad / weight

    for p, c in chunks:
        for hop in hops:
            with mark("w_ag"):
                gather(p, c, hop).wait_recv()
            share(p, c, hop).start()
    for p in range(pairs):
        for q in range(2):
            half = slice(q * n, (q + 1) * n)
            probe_out[2 * p + col, q] = probe_ref[pairs + p, q] - probe_rate * fin[p, half] / tiles
    for p in range(pairs):
        with mark("w_share"):
            for c in range(CUTS):
                for hop in range(group):
                    share(p, c, hop).wait_recv()
        for q in range(2):
            half = slice(q * n, (q + 1) * n)
            probe_out[2 * p + 1 - col, q] = probe_ref[p, q] - probe_rate * fin_other[p, half] / tiles

    with mark("w_sends"):
        to_mate.wait_send()
        for side, has in sent:
            for i in range(len(strips)):
                pl.when(has)(halo(side, i).wait_send)
        for side, has in got:
            for i in range(len(strips)):
                pl.when(has)(relay(side, i).wait_send)
        for p in range(pairs):
            to_partner(p).wait_send()
        for j in range(3):
            across(j).wait_send()
        pl.when(has_up)(edge_up.wait_send)
        pl.when(has_down)(edge_down.wait_send)
        for p, c in chunks:
            for hop in hops:
                scatter(p, c, hop).wait_send()
                gather(p, c, hop).wait_send()
            for r in range(len(ways)):
                exchange(r, p, c).wait_send()
            for hop in range(group):
                share(p, c, hop).wait_send()


def finish(obj_ref, probe_ref, obj_out, probe_out, sem):
    copies = [pltpu.make_async_copy(obj_ref, obj_out, sem.at[0]), pltpu.make_async_copy(probe_ref, probe_out, sem.at[1])]
    for copy in copies:
        copy.start()
    for copy in copies:
        copy.wait()


def body(rows, object_field, probe, patterns, offsets, counts):
    modes, _, n, _ = probe.shape
    slots = patterns.shape[2]
    pairs = modes // 2
    group, ways = plan(rows)
    rounds = max(1, len(ways))
    far_hops = max(1, group - 1)
    slab = 2 * n // group
    tables = jnp.asarray(dft_tables(n))
    vmem = pl.BlockSpec(memory_space=pltpu.VMEM)
    hbm = pl.BlockSpec(memory_space=pltpu.HBM)
    dma = pltpu.SemaphoreType.DMA
    wide, tall = (slots, 2 * n, modes * n), (slots, modes * n, 2 * n)
    outs = (
        jax.ShapeDtypeStruct(object_field.shape, F32),
        jax.ShapeDtypeStruct(probe.shape, F32),
    )
    results = pl.pallas_call(
        functools.partial(kernel, rows, modes, slots, n),
        out_shape=outs,
        in_specs=[hbm] * 6,
        out_specs=(vmem, vmem),
        scratch_shapes=[
            pltpu.SMEM(offsets.shape, jnp.int32),
            pltpu.SMEM(counts.shape, jnp.int32),
            pltpu.VMEM(probe.shape, F32),
            pltpu.VMEM(patterns.shape, F32),
            pltpu.VMEM(tables.shape, BF16),
            pltpu.VMEM((3, 3, 2, n, n), F32),
            pltpu.VMEM(tall, BF16),
            pltpu.VMEM(tall, BF16),
            pltpu.VMEM(wide, BF16),
            pltpu.VMEM(wide, BF16),
            pltpu.VMEM(wide, F32),
            pltpu.VMEM((slots, 2 * n, 2 * n), BF16),
            pltpu.VMEM((slots, 2 * n, 2 * n), BF16),
            pltpu.VMEM((slots, 2, n, n), F32),
            pltpu.VMEM((slots, 2, n, n), F32),
            pltpu.VMEM((3, 2, n, n), F32),
            pltpu.VMEM((3, 2, n, n), F32),
            pltpu.VMEM((3, 2, n, n), F32),
            pltpu.VMEM((2, 2, n, n), F32),
            pltpu.VMEM((modes, 2 * n, n), F32),
            pltpu.VMEM((pairs, 2 * n, n), F32),
            pltpu.VMEM((pairs, 2 * n, n), F32),
            pltpu.VMEM((far_hops, pairs, slab, n), F32),
            pltpu.VMEM((rounds, pairs, slab, n), F32),
            pltpu.VMEM((rounds, pairs, slab, n), F32),
            pltpu.VMEM((pairs, 2 * n, n), F32),
            pltpu.VMEM((pairs, 2 * n, n), F32),
            dma((5 + modes,)),
            dma((1,)), dma((1,)),
            dma((2, 2 * STRIPS)), dma((2, 2 * STRIPS)),
            dma((2, 2 * STRIPS)), dma((2, 2 * STRIPS)),
            dma((3,)), dma((3,)),
            dma((2,)), dma((2,)),
            dma((pairs,)), dma((pairs,)),
            dma((far_hops, pairs, CUTS)), dma((far_hops, pairs, CUTS)),
            dma((rounds, pairs, CUTS)), dma((rounds, pairs, CUTS)),
            dma((far_hops, pairs, CUTS)), dma((far_hops, pairs, CUTS)),
            dma((group, pairs, CUTS)), dma((group, pairs, CUTS)),
        ],
        compiler_params=pltpu.CompilerParams(
            collective_id=0, has_side_effects=True, vmem_limit_bytes=24 << 20
        ),
    )(*[pltpu.with_memory_space_constraint(x, pltpu.HBM) for x in (offsets,)], counts, *[pltpu.with_memory_space_constraint(x, pltpu.HBM) for x in (object_field, probe, patterns, tables)])
    return pl.pallas_call(
        finish,
        out_shape=outs,
        in_specs=[vmem] * 2,
        out_specs=(hbm, hbm),
        scratch_shapes=[dma((2,))],
        compiler_params=pltpu.CompilerParams(vmem_limit_bytes=4 << 20),
    )(*results)


def solution(mesh):
    placed = (
        P(None, ("tilt", "row"), "col"),
        P("tilt", None, None, None),
        P(("tilt", "row"), "col", None, None, None),
        P(("tilt", "row"), "col", None, None),
        P(("tilt", "row"), "col"),
    )
    return jax.shard_map(
        functools.partial(body, mesh.shape["row"]),
        mesh=mesh,
        in_specs=placed,
        out_specs=(P(None, ("tilt", "row"), "col"), P("tilt", None, None, None)),
        check_vma=False,
    )
```

```python
import contextlib
import functools

import jax
import jax.numpy as jnp
import numpy as np
from jax import lax
from jax.experimental import pallas as pl
from jax.experimental.pallas import tpu as pltpu
from jax.sharding import PartitionSpec as P

MESH = pl.DeviceIdType.MESH
F32 = jnp.float32
BF16 = jnp.bfloat16

object_rate = 1.0
probe_rate = 1.0
epsilon = 1e-06


def mark(name):
    return contextlib.nullcontext()


def split_table(table):
    high = table.astype(jnp.bfloat16)
    low = (table - high.astype(np.float64)).astype(jnp.bfloat16)
    return high, low


def dft_tables(length):
    counter = np.arange(length)
    product = counter[:, None] * counter[None, :] % length
    angle = -2.0 * np.pi / length * product
    c, s = np.cos(angle) / np.sqrt(length), np.sin(angle) / np.sqrt(length)
    right = np.block([[c, s], [-s, c]])
    left = right.T
    return np.stack([*split_table(right), *split_table(left)])


def split(x):
    high = x.astype(BF16)
    return high, (x - high.astype(F32)).astype(BF16)


def dot(a, b):
    return jnp.dot(a, b, preferred_element_type=F32)


def plan(rows):
    assert rows & (rows - 1) == 0
    group = min(4, rows)
    ways = []
    while group << len(ways) < rows:
        ways.append(group << len(ways))
    return group, ways


CUTS = 2
STRIPS = (2, 2, 2, 1, 1)


def kernel(
    rows, modes, slots, width,
    off_hbm, cnt_hbm, obj_hbm, probe_hbm, pat_hbm, tab_hbm,
    obj_out, probe_out,
    off_ref, cnt_ref, probe_ref, pat_ref, tab_ref,
    frame, xh, xl, yh, yl, far, vh, vl, win, gacc,
    gown, gpar, grecv, gnear, gfar, term, tpart, acc, pieces, part, swapped, fin, fin_other,
    load, hm_send, hm_recv, n_send, n_recv, f_send, f_recv, r_send, r_recv, g_send, g_recv,
    e_send, e_recv, t_send, t_recv, rs_send, rs_recv, x_send, x_recv, ag_send, ag_recv, o_send, o_recv,
):
    me = lax.axis_index("row")
    col = lax.axis_index("col")
    n = width
    tiles = rows * 2
    pairs = modes // 2
    group, ways = plan(rows)
    slab = 2 * n // group
    chunk = slab // CUTS
    mate = {"col": 1 - col}
    odd = lax.rem(me, 2)
    near_at, far_at = 2 - 2 * odd, 2 * odd
    near, far_row = me + 1 - 2 * odd, me - 1 + 2 * odd
    has_far = jnp.logical_and(far_row >= 0, far_row < rows)
    seat = lax.rem(me, group)

    def flip(index, bit):
        return jnp.where(lax.rem(index // bit, 2) == 0, index + bit, index - bit)

    def hop_to(index, hop):
        for b in range(hop.bit_length()):
            if hop >> b & 1:
                index = flip(index, 1 << b)
        return index

    def mode_at(spot):
        return 2 * spot + 1 - col if spot < pairs else 2 * (spot - pairs) + col

    obj_load = pltpu.make_async_copy(obj_hbm, frame.at[1, 1], load.at[0])
    loads = [
        pltpu.make_async_copy(off_hbm, off_ref, load.at[1]),
        pltpu.make_async_copy(cnt_hbm, cnt_ref, load.at[2]),
        pltpu.make_async_copy(pat_hbm, pat_ref, load.at[3]),
        pltpu.make_async_copy(tab_hbm, tab_ref, load.at[4]),
    ]
    probes = [pltpu.make_async_copy(probe_hbm.at[mode_at(j)], probe_ref.at[j], load.at[5]) for j in range(modes)]
    all_probes = pltpu.make_async_copy(probe_hbm, probe_ref, load.at[5])

    barrier = pltpu.get_barrier_semaphore()

    def greet(to):
        pl.semaphore_signal(barrier, inc=1, device_id=to, device_id_type=MESH)

    peers = [hop_to(me, hop) for hop in range(1, group)] + [flip(me, way) for way in ways]
    pl.when(has_far)(lambda: greet({"row": far_row}))
    for peer in peers:
        greet({"row": peer})
    greet(mate)
    for copy in [obj_load] + probes + loads:
        copy.start()
    with mark("w_barrier"):
        pl.semaphore_wait(
            barrier, 1 + has_far.astype(jnp.int32) + len(peers)
        )

    def remote(src, dst, send, recv, to):
        return pltpu.make_async_remote_copy(
            src_ref=src, dst_ref=dst, send_sem=send, recv_sem=recv, device_id=to, device_id_type=MESH
        )

    seen = 2 * col
    mine = 2 - 2 * col
    unit = 2 * n // sum(STRIPS)
    starts = [unit * sum(STRIPS[:i]) for i in range(len(STRIPS) + 1)]
    strips = [pl.ds(starts[i], starts[i + 1] - starts[i]) for i in range(len(STRIPS))]
    to_mate = remote(obj_hbm, frame.at[1, seen], hm_send.at[0], hm_recv.at[0], mate)

    def to_near(i, at=None):
        at = strips[i] if at is None else at
        return remote(obj_hbm.at[at], frame.at[far_at, 1, at], n_send.at[0], n_recv.at[i], {"row": near})

    def to_far(i, at=None):
        at = strips[i] if at is None else at
        return remote(obj_hbm.at[at], frame.at[near_at, 1, at], f_send.at[0], f_recv.at[i], {"row": far_row})

    def relay(block, kind, at):
        return remote(
            frame.at[block, 1, at], frame.at[block, seen, at], r_send.at[kind], r_recv.at[kind], mate
        )

    whole = pl.ds(0, 2 * n)
    last = len(STRIPS)
    for i in range(last):
        pl.when(has_far)(to_far(i).start)
        to_near(i).start()
    to_mate.start()

    zero = jnp.zeros((2 * n, n), F32)
    for j in range(3):
        frame[j, seen] = zero

    @pl.when(jnp.logical_not(has_far))
    def _():
        frame[far_at, 1] = zero
        frame[far_at, mine] = zero
        gfar[...] = zero

    with mark("w_load"):
        all_probes.wait()
    power = jnp.zeros((n, n), F32)
    for k in range(modes):
        power = power + (probe_ref[k, 0] * probe_ref[k, 0] + probe_ref[k, 1] * probe_ref[k, 1])
    weight = jnp.max(power) + epsilon

    with mark("w_halo"):
        def far_strip(i):
            @pl.when(has_far)
            def _():
                to_far(i).wait_recv()
                relay(far_at, 1, strips[i]).start()

        def near_strip(i):
            to_near(i).wait_recv()
            relay(near_at, 0, strips[i]).start()

        for i in range(last):
            near_strip(i)
            far_strip(i)

    obj_load.wait()
    for copy in loads:
        copy.wait()
    to_mate.wait_recv()
    with mark("w_relay"):
        relay(near_at, 0, whole).wait_recv()
        pl.when(has_far)(relay(far_at, 1, whole).wait_recv)

    r_hi, r_lo, l_hi, l_lo = (tab_ref.at[t] for t in range(4))
    row_id = lax.broadcasted_iota(jnp.int32, (n, n), 0)
    lane_id = lax.broadcasted_iota(jnp.int32, (n, n), 1)

    def place(s):
        oy, ox = off_ref[0, 0, s, 0], off_ref[0, 0, s, 1]
        by, bx = oy // n, ox // n
        return by, bx, oy - by * n, ox - bx * n

    for s in range(slots):
        by, bx, sy, sx = place(s)
        by2, bx2 = jnp.minimum(by + 1, 2), jnp.minimum(bx + 1, 2)
        for q in range(2):
            half = slice(q * n, (q + 1) * n)
            upper = jnp.where(lane_id >= sx, frame[by, bx, half], frame[by, bx2, half])
            lower = jnp.where(lane_id >= sx, frame[by2, bx, half], frame[by2, bx2, half])
            packed = jnp.where(row_id >= sy, upper, lower)
            packed = pltpu.roll(packed, lax.rem(n - sy, n), 0)
            win[s, q] = pltpu.roll(packed, lax.rem(n - sx, n), 1)
        for k in range(modes):
            wr, wi = win[s, 0], win[s, 1]
            pr, pi = probe_ref[k, 0], probe_ref[k, 1]
            for q, value in enumerate((pr * wr - pi * wi, pr * wi + pi * wr)):
                hi, lo = split(value)
                xh[s, k * n : (k + 1) * n, q * n : (q + 1) * n] = hi
                xl[s, k * n : (k + 1) * n, q * n : (q + 1) * n] = lo
        for k in range(modes):
            a_hi, a_lo = xh[s, k * n : (k + 1) * n, :], xl[s, k * n : (k + 1) * n, :]
            y = dot(a_hi, r_hi[...]) + dot(a_lo, r_hi[...]) + dot(a_hi, r_lo[...])
            for q in range(2):
                hi, lo = split(y[:, q * n : (q + 1) * n])
                yh[s, q * n : (q + 1) * n, k * n : (k + 1) * n] = hi
                yl[s, q * n : (q + 1) * n, k * n : (k + 1) * n] = lo
        for p in range(modes // 2):
            cols = slice(2 * p * n, 2 * (p + 1) * n)
            b_hi, b_lo = yh[s, :, cols], yl[s, :, cols]
            far[s, :, cols] = dot(l_hi[...], b_hi) + dot(l_lo[...], b_hi) + dot(l_hi[...], b_lo)
        level = jnp.zeros((n, n), F32)
        for k in range(modes):
            cols = slice(k * n, (k + 1) * n)
            level = level + far[s, :n, cols] * far[s, :n, cols] + far[s, n:, cols] * far[s, n:, cols]
        live = (s < cnt_ref[0, 0]).astype(F32)
        misfit = live * (level - pat_ref[0, 0, s])
        for k in range(modes):
            for q in range(2):
                spot = (s, slice(q * n, (q + 1) * n), slice(k * n, (k + 1) * n))
                hi, lo = split(misfit * far[spot])
                yh[spot] = hi
                yl[spot] = lo

    def to_partner(p):
        return remote(term.at[p], tpart.at[p], t_send.at[0], t_recv.at[p], mate)

    def rows_of(owner, c):
        return pl.ds(pl.multiple_of(owner * slab + c * chunk, 8), chunk)

    def scatter(p, c, hop):
        return remote(
            acc.at[p, rows_of(hop_to(seat, hop), c)], pieces.at[p, c, hop - 1],
            rs_send.at[0], rs_recv.at[p, c], {"row": hop_to(me, hop)},
        )

    hops = list(range(1, group))
    for b in range(modes // 2):
        cols = slice(2 * b * n, 2 * (b + 1) * n)
        for s in range(slots):
            b_hi, b_lo = yh[s, :, cols], yl[s, :, cols]
            v = dot(r_hi[...], b_hi) + dot(r_lo[...], b_hi) + dot(r_hi[...], b_lo)
            for m in range(2):
                for q in range(2):
                    hi, lo = split(v[q * n : (q + 1) * n, m * n : (m + 1) * n])
                    vh[s, m * n : (m + 1) * n, q * n : (q + 1) * n] = hi
                    vl[s, m * n : (m + 1) * n, q * n : (q + 1) * n] = lo
        for m in range(2):
            k = 2 * b + m
            for s in range(slots):
                a_hi, a_lo = vh[s, m * n : (m + 1) * n, :], vl[s, m * n : (m + 1) * n, :]
                back = dot(a_hi, l_hi[...]) + dot(a_lo, l_hi[...]) + dot(a_hi, l_lo[...])
                br, bi = back[:, :n], back[:, n:]
                pr, pi = probe_ref[k, 0], probe_ref[k, 1]
                gr, gi = pr * br + pi * bi, pr * bi - pi * br
                wr, wi = win[s, 0], win[s, 1]
                tr, ti = wr * br + wi * bi, wr * bi - wi * br
                if k == 0:
                    gacc[s, 0], gacc[s, 1] = gr, gi
                else:
                    gacc[s, 0], gacc[s, 1] = gacc[s, 0] + gr, gacc[s, 1] + gi
                if s == 0:
                    term[k, :n], term[k, n:] = tr, ti
                else:
                    term[k, :n], term[k, n:] = term[k, :n] + tr, term[k, n:] + ti
            if k < pairs:
                to_partner(k).start()
            else:
                p = k - pairs
                with mark("w_partner"):
                    to_partner(p).wait_recv()
                acc[p] = term[k] + tpart[p]
                for c in range(CUTS):
                    for hop in hops:
                        scatter(p, c, hop).start()

    def across(j):
        return remote(gpar.at[j], grecv.at[j], g_send.at[0], g_recv.at[j], mate)

    for q in range(2):
        own = [jnp.zeros((n, n), F32)] * 3
        par = [jnp.zeros((n, n), F32)] * 3
        for s in range(slots):
            by, bx, sy, sx = place(s)
            g = pltpu.roll(pltpu.roll(gacc[s, q], sy, 0), sx, 1)
            low_x, low_y = (lane_id >= sx).astype(F32), (row_id >= sy).astype(F32)

            def side_of(block, at, low):
                return (block == at).astype(F32) * low + (block == at + 1).astype(F32) * (1.0 - low)

            g_own, g_par = g * side_of(1, bx, low_x), g * side_of(mine, bx, low_x)
            for j in range(3):
                mask = side_of(j, by, low_y)
                own[j] = own[j] + g_own * mask
                par[j] = par[j] + g_par * mask
        for j in range(3):
            gown[j, q * n : (q + 1) * n] = own[j]
            gpar[j, q * n : (q + 1) * n] = par[j]
    edge_far = remote(gown.at[far_at], gfar, e_send.at[0], e_recv.at[0], {"row": far_row})
    edge_near = remote(gown.at[near_at], gnear, e_send.at[1], e_recv.at[1], {"row": near})
    for j in (far_at, near_at, 1):
        across(j).start()
    with mark("w_across"):
        for j in (far_at, near_at):
            across(j).wait_recv()
            gown[j] = gown[j] + grecv[j]

    chunks = [(p, c) for p in range(pairs) for c in range(CUTS)]

    def exchange(r, p, c):
        return remote(
            part.at[p, c, r], swapped.at[p, c, r], x_send.at[0], x_recv.at[p, c, r], {"row": flip(me, ways[r])}
        )

    def gather(p, c, hop):
        here = fin.at[p, rows_of(seat, c)]
        return remote(here, here, ag_send.at[0], ag_recv.at[p, c], {"row": hop_to(me, hop)})

    def share(p, c, hop):
        at = rows_of(hop_to(seat, hop), c)
        return remote(fin.at[p, at], fin_other.at[p, at], o_send.at[0], o_recv.at[p], mate)

    def settle(r, p, c, total):
        if r < len(ways):
            part[p, c, r] = total
            exchange(r, p, c).start()
        else:
            fin[p, rows_of(seat, c)] = total
            for hop in hops:
                gather(p, c, hop).start()
            share(p, c, 0).start()

    def all_of(ref, send, recv):
        return remote(ref, ref, send, recv, mate)

    for p, c in chunks:
        total = acc[p, rows_of(seat, c)]
        with mark("w_rs"):
            all_of(pieces.at[p, c], rs_send.at[0], rs_recv.at[p, c]).wait_recv()
        for hop in hops:
            total = total + pieces[p, c, hop - 1]
        settle(0, p, c, total)
        if (p, c) == chunks[0]:
            edge_near.start()
    pl.when(has_far)(edge_far.start)
    for r in range(len(ways)):
        for p, c in chunks:
            with mark("w_xc"):
                exchange(r, p, c).wait_recv()
            settle(r + 1, p, c, part[p, c, r] + swapped[p, c, r])

    for p, c in chunks:
        with mark("w_ag"):
            all_of(pieces.at[p, c], ag_send.at[0], ag_recv.at[p, c]).wait_recv()
        for hop in hops:
            share(p, c, hop).start()
    for p in range(pairs):
        for q in range(2):
            half = slice(q * n, (q + 1) * n)
            probe_out[2 * p + col, q] = probe_ref[pairs + p, q] - probe_rate * fin[p, half] / tiles
    with mark("w_edge"):
        across(1).wait_recv()
        edge_near.wait_recv()
        pl.when(has_far)(edge_far.wait_recv)
    for q in range(2):
        half = slice(q * n, (q + 1) * n)
        grad = gown[1, half] + grecv[1, half] + gnear[half] + gfar[half]
        obj_out[half] = frame[1, 1, half] - object_rate * grad / weight

    for p in range(pairs):
        with mark("w_share"):
            all_of(fin_other.at[p], o_send.at[0], o_recv.at[p]).wait_recv()
        for q in range(2):
            half = slice(q * n, (q + 1) * n)
            probe_out[2 * p + 1 - col, q] = probe_ref[p, q] - probe_rate * fin_other[p, half] / tiles

    with mark("w_sends"):
        to_mate.wait_send()
        to_near(0, whole).wait_send()
        pl.when(has_far)(to_far(0, whole).wait_send)
        relay(near_at, 0, whole).wait_send()
        pl.when(has_far)(relay(far_at, 1, whole).wait_send)
        pl.when(has_far)(edge_far.wait_send)
        edge_near.wait_send()
        for ref, send, recv in (
            (tpart, t_send, t_recv.at[0]), (gpar, g_send, g_recv.at[0]), (pieces, rs_send, rs_recv.at[0, 0]),
            (pieces, ag_send, ag_recv.at[0, 0]), (fin_other, o_send, o_recv.at[0]),
        ):
            all_of(ref, send.at[0], recv).wait_send()
        if ways:
            all_of(part, x_send.at[0], x_recv.at[0, 0, 0]).wait_send()


def finish(obj_ref, probe_ref, obj_out, probe_out, sem):
    copies = [pltpu.make_async_copy(obj_ref, obj_out, sem.at[0])]
    for k in range(probe_ref.shape[0]):
        copies.append(pltpu.make_async_copy(probe_ref.at[k], probe_out.at[k], sem.at[k + 1]))
    for copy in copies:
        copy.start()
    for copy in copies:
        copy.wait()


def body(rows, object_field, probe, patterns, offsets, counts):
    modes, _, n, _ = probe.shape
    slots = patterns.shape[2]
    pairs = modes // 2
    assert rows > 1
    group, ways = plan(rows)
    block = object_field.reshape(2 * n, n)
    rounds = max(1, len(ways))
    chunk = 2 * n // group // CUTS
    tables = jnp.asarray(dft_tables(n))
    vmem = pl.BlockSpec(memory_space=pltpu.VMEM)
    hbm = pl.BlockSpec(memory_space=pltpu.HBM)
    dma = pltpu.SemaphoreType.DMA
    wide, tall = (slots, 2 * n, modes * n), (slots, modes * n, 2 * n)
    outs = (
        jax.ShapeDtypeStruct(block.shape, F32),
        jax.ShapeDtypeStruct(probe.shape, F32),
    )
    results = pl.pallas_call(
        functools.partial(kernel, rows, modes, slots, n),
        out_shape=outs,
        in_specs=[hbm] * 6,
        out_specs=(vmem, vmem),
        scratch_shapes=[
            pltpu.SMEM(offsets.shape, jnp.int32),
            pltpu.SMEM(counts.shape, jnp.int32),
            pltpu.VMEM(probe.shape, F32),
            pltpu.VMEM(patterns.shape, F32),
            pltpu.VMEM(tables.shape, BF16),
            pltpu.VMEM((3, 3, 2 * n, n), F32),
            pltpu.VMEM(tall, BF16),
            pltpu.VMEM(tall, BF16),
            pltpu.VMEM(wide, BF16),
            pltpu.VMEM(wide, BF16),
            pltpu.VMEM(wide, F32),
            pltpu.VMEM((slots, 2 * n, 2 * n), BF16),
            pltpu.VMEM((slots, 2 * n, 2 * n), BF16),
            pltpu.VMEM((slots, 2, n, n), F32),
            pltpu.VMEM((slots, 2, n, n), F32),
            pltpu.VMEM((3, 2 * n, n), F32),
            pltpu.VMEM((3, 2 * n, n), F32),
            pltpu.VMEM((3, 2 * n, n), F32),
            pltpu.VMEM((2 * n, n), F32),
            pltpu.VMEM((2 * n, n), F32),
            pltpu.VMEM((modes, 2 * n, n), F32),
            pltpu.VMEM((pairs, 2 * n, n), F32),
            pltpu.VMEM((pairs, 2 * n, n), F32),
            pltpu.VMEM((pairs, CUTS, group - 1, chunk, n), F32),
            pltpu.VMEM((pairs, CUTS, rounds, chunk, n), F32),
            pltpu.VMEM((pairs, CUTS, rounds, chunk, n), F32),
            pltpu.VMEM((pairs, 2 * n, n), F32),
            pltpu.VMEM((pairs, 2 * n, n), F32),
            dma((6,)),
            dma((1,)), dma((1,)),
            dma((1,)), dma((len(STRIPS),)),
            dma((1,)), dma((len(STRIPS),)),
            dma((2,)), dma((2,)),
            dma((1,)), dma((3,)),
            dma((2,)), dma((2,)),
            dma((1,)), dma((pairs,)),
            dma((1,)), dma((pairs, CUTS)),
            dma((1,)), dma((pairs, CUTS, rounds)),
            dma((1,)), dma((pairs, CUTS)),
            dma((1,)), dma((pairs,)),
        ],
        compiler_params=pltpu.CompilerParams(
            collective_id=0, has_side_effects=True, vmem_limit_bytes=24 << 20
        ),
    )(*[pltpu.with_memory_space_constraint(x, pltpu.HBM) for x in (offsets,)], counts, *[pltpu.with_memory_space_constraint(x, pltpu.HBM) for x in (block, probe, patterns, tables)])
    new_block, new_probe = pl.pallas_call(
        finish,
        out_shape=outs,
        in_specs=[vmem] * 2,
        out_specs=(hbm, hbm),
        scratch_shapes=[dma((1 + modes,))],
        compiler_params=pltpu.CompilerParams(vmem_limit_bytes=4 << 20),
    )(*results)
    return new_block.reshape(object_field.shape), new_probe


def solution(mesh):
    placed = (
        P(None, ("tilt", "row"), "col"),
        P("tilt", None, None, None),
        P(("tilt", "row"), "col", None, None, None),
        P(("tilt", "row"), "col", None, None),
        P(("tilt", "row"), "col"),
    )
    return jax.shard_map(
        functools.partial(body, mesh.shape["row"]),
        mesh=mesh,
        in_specs=placed,
        out_specs=(P(None, ("tilt", "row"), "col"), P("tilt", None, None, None)),
        check_vma=False,
    )
```

```python
import contextlib
import functools

import jax
import jax.numpy as jnp
import numpy as np
from jax import lax
from jax.experimental import pallas as pl
from jax.experimental.pallas import tpu as pltpu
from jax.sharding import PartitionSpec as P

MESH = pl.DeviceIdType.MESH
F32 = jnp.float32
BF16 = jnp.bfloat16

object_rate = 1.0
probe_rate = 1.0
epsilon = 1e-06


def mark(name):
    return contextlib.nullcontext()


def split_table(table):
    high = table.astype(jnp.bfloat16)
    low = (table - high.astype(np.float64)).astype(jnp.bfloat16)
    return high, low


def dft_tables(length):
    counter = np.arange(length)
    product = counter[:, None] * counter[None, :] % length
    angle = -2.0 * np.pi / length * product
    c, s = np.cos(angle) / np.sqrt(length), np.sin(angle) / np.sqrt(length)
    right = np.block([[c, s], [-s, c]])
    left = right.T
    return np.stack([*split_table(right), *split_table(left)])


def split(x):
    high = x.astype(BF16)
    return high, (x - high.astype(F32)).astype(BF16)


def dot(a, b):
    return jnp.dot(a, b, preferred_element_type=F32)


def right3(a_hi, a_lo, hi, lo):
    m = a_hi.shape[0]
    both = dot(jnp.concatenate([a_hi, a_lo], 0), hi)
    return both[:m] + both[m:] + dot(a_hi, lo)


def left3(hi, lo, b_hi, b_lo):
    m = hi.shape[0]
    both = dot(jnp.concatenate([hi, lo], 0), b_hi)
    return both[:m] + both[m:] + dot(hi, b_lo)


def plan(rows):
    assert rows & (rows - 1) == 0
    group = min(4, rows)
    ways = []
    while group << len(ways) < rows:
        ways.append(group << len(ways))
    return group, ways


CUTS = 2
STRIPS = (2, 2, 2, 1, 1)


def kernel(
    rows, modes, slots, width,
    off_hbm, cnt_hbm, obj_hbm, probe_hbm, pat_hbm, tab_hbm,
    obj_out, probe_out,
    off_ref, cnt_ref, probe_ref, pat_ref, tab_ref,
    frame, xh, xl, yh, yl, far, vh, vl, win, gacc,
    gown, gpar, grecv, gnear, gfar, gvia, term, tpart, acc, pieces, part, swapped, fin, fin_other,
    load, hm_send, hm_recv, n_send, n_recv, f_send, f_recv, p_send, r_send, r_recv, g_send, g_recv,
    e_send, e_recv, t_send, t_recv, rs_send, rs_recv, x_send, x_recv, ag_send, ag_recv, o_send, o_recv,
):
    me = lax.axis_index("row")
    col = lax.axis_index("col")
    n = width
    tiles = rows * 2
    pairs = modes // 2
    group, ways = plan(rows)
    slab = 2 * n // group
    chunk = slab // CUTS
    mate = {"col": 1 - col}
    odd = lax.rem(me, 2)
    near_at, far_at = 2 - 2 * odd, 2 * odd
    near, far_row, beyond, behind = me + 1 - 2 * odd, me - 1 + 2 * odd, me - 2 + 4 * odd, me + 2 - 4 * odd
    has_far = jnp.logical_and(far_row >= 0, far_row < rows)
    direct = jnp.logical_and(has_far, col == 0)
    passes = jnp.logical_and(jnp.logical_and(behind >= 0, behind < rows), col == 1)
    passed = jnp.logical_and(has_far, col == 1)
    seat = lax.rem(me, group)

    def flip(index, bit):
        return jnp.where(lax.rem(index // bit, 2) == 0, index + bit, index - bit)

    def hop_to(index, hop):
        for b in range(hop.bit_length()):
            if hop >> b & 1:
                index = flip(index, 1 << b)
        return index

    def mode_at(spot):
        return 2 * spot + 1 - col if spot < pairs else 2 * (spot - pairs) + col

    obj_load = pltpu.make_async_copy(obj_hbm, frame.at[1, 1], load.at[0])
    loads = [
        pltpu.make_async_copy(off_hbm, off_ref, load.at[1]),
        pltpu.make_async_copy(cnt_hbm, cnt_ref, load.at[2]),
        pltpu.make_async_copy(pat_hbm, pat_ref, load.at[3]),
        pltpu.make_async_copy(tab_hbm, tab_ref, load.at[4]),
    ]
    probes = [pltpu.make_async_copy(probe_hbm.at[mode_at(j)], probe_ref.at[j], load.at[5]) for j in range(modes)]
    all_probes = pltpu.make_async_copy(probe_hbm, probe_ref, load.at[5])

    barrier = pltpu.get_barrier_semaphore()

    def greet(to):
        pl.semaphore_signal(barrier, inc=1, device_id=to, device_id_type=MESH)

    peers = [hop_to(me, hop) for hop in range(1, group)] + [flip(me, way) for way in ways]
    pl.when(has_far)(lambda: greet({"row": far_row}))
    pl.when(passed)(lambda: greet({"row": beyond}))
    pl.when(passes)(lambda: greet({"row": behind}))
    for peer in peers:
        greet({"row": peer})
    greet(mate)
    for copy in [obj_load] + probes + loads:
        copy.start()
    with mark("w_barrier"):
        pl.semaphore_wait(
            barrier, 1 + has_far.astype(jnp.int32) + passed.astype(jnp.int32) + passes.astype(jnp.int32) + len(peers)
        )

    def remote(src, dst, send, recv, to):
        return pltpu.make_async_remote_copy(
            src_ref=src, dst_ref=dst, send_sem=send, recv_sem=recv, device_id=to, device_id_type=MESH
        )

    seen = 2 * col
    mine = 2 - 2 * col
    unit = 2 * n // sum(STRIPS)
    starts = [unit * sum(STRIPS[:i]) for i in range(len(STRIPS) + 1)]
    strips = [pl.ds(starts[i], starts[i + 1] - starts[i]) for i in range(len(STRIPS))]
    to_mate = remote(obj_hbm, frame.at[1, seen], hm_send.at[0], hm_recv.at[0], mate)

    def to_near(i, at=None):
        at = strips[i] if at is None else at
        return remote(obj_hbm.at[at], frame.at[far_at, 1, at], n_send.at[0], n_recv.at[i], {"row": near})

    def to_far(i, at=None):
        at = strips[i] if at is None else at
        return remote(obj_hbm.at[at], frame.at[near_at, 1, at], f_send.at[0], f_recv.at[i], {"row": far_row})

    def pass_on(i, at=None):
        at = strips[i] if at is None else at
        return remote(
            frame.at[near_at, 1, at], frame.at[far_at, 1, at], p_send.at[0], f_recv.at[i], {"row": behind}
        )

    def relay(block, kind, at):
        return remote(
            frame.at[block, 1, at], frame.at[block, seen, at], r_send.at[kind], r_recv.at[kind], mate
        )

    whole = pl.ds(0, 2 * n)
    last = len(STRIPS)
    for i in range(last):
        to_near(i).start()
    for i in range(last):
        pl.when(direct)(to_far(i).start)
    to_mate.start()

    zero = jnp.zeros((2 * n, n), F32)
    for j in range(3):
        frame[j, seen] = zero

    @pl.when(jnp.logical_not(has_far))
    def _():
        frame[far_at, 1] = zero
        frame[far_at, mine] = zero

    @pl.when(jnp.logical_not(direct))
    def _():
        gfar[...] = zero

    with mark("w_load"):
        all_probes.wait()
    power = jnp.zeros((n, n), F32)
    for k in range(modes):
        power = power + (probe_ref[k, 0] * probe_ref[k, 0] + probe_ref[k, 1] * probe_ref[k, 1])
    weight = jnp.max(power) + epsilon

    with mark("w_halo"):
        def far_strip(i):
            @pl.when(has_far)
            def _():
                to_far(i).wait_recv()
                relay(far_at, 1, strips[i]).start()

        def near_strip(i):
            to_near(i).wait_recv()
            pl.when(passes)(pass_on(i).start)
            relay(near_at, 0, strips[i]).start()

        for i in range(last):
            near_strip(i)
        for i in range(last):
            far_strip(i)

    obj_load.wait()
    for copy in loads:
        copy.wait()
    to_mate.wait_recv()
    with mark("w_relay"):
        relay(near_at, 0, whole).wait_recv()
        pl.when(has_far)(relay(far_at, 1, whole).wait_recv)

    r_hi, r_lo, l_hi, l_lo = (tab_ref.at[t] for t in range(4))
    row_id = lax.broadcasted_iota(jnp.int32, (n, n), 0)
    lane_id = lax.broadcasted_iota(jnp.int32, (n, n), 1)

    def place(s):
        oy, ox = off_ref[0, 0, s, 0], off_ref[0, 0, s, 1]
        by, bx = oy // n, ox // n
        return by, bx, oy - by * n, ox - bx * n

    for s in range(slots):
        by, bx, sy, sx = place(s)
        by2, bx2 = jnp.minimum(by + 1, 2), jnp.minimum(bx + 1, 2)
        for q in range(2):
            half = slice(q * n, (q + 1) * n)
            upper = jnp.where(lane_id >= sx, frame[by, bx, half], frame[by, bx2, half])
            lower = jnp.where(lane_id >= sx, frame[by2, bx, half], frame[by2, bx2, half])
            packed = jnp.where(row_id >= sy, upper, lower)
            packed = pltpu.roll(packed, lax.rem(n - sy, n), 0)
            win[s, q] = pltpu.roll(packed, lax.rem(n - sx, n), 1)
    for s in range(slots):
        for k in range(modes):
            wr, wi = win[s, 0], win[s, 1]
            pr, pi = probe_ref[k, 0], probe_ref[k, 1]
            for q, value in enumerate((pr * wr - pi * wi, pr * wi + pi * wr)):
                hi, lo = split(value)
                xh[s, k * n : (k + 1) * n, q * n : (q + 1) * n] = hi
                xl[s, k * n : (k + 1) * n, q * n : (q + 1) * n] = lo
    for s in range(slots):
        for k in range(modes):
            a_hi, a_lo = xh[s, k * n : (k + 1) * n, :], xl[s, k * n : (k + 1) * n, :]
            y = right3(a_hi, a_lo, r_hi[...], r_lo[...])
            for q in range(2):
                hi, lo = split(y[:, q * n : (q + 1) * n])
                yh[s, q * n : (q + 1) * n, k * n : (k + 1) * n] = hi
                yl[s, q * n : (q + 1) * n, k * n : (k + 1) * n] = lo
    for s in range(slots):
        for p in range(modes // 2):
            cols = slice(2 * p * n, 2 * (p + 1) * n)
            b_hi, b_lo = yh[s, :, cols], yl[s, :, cols]
            far[s, :, cols] = left3(l_hi[...], l_lo[...], b_hi, b_lo)
    for s in range(slots):
        level = jnp.zeros((n, n), F32)
        for k in range(modes):
            cols = slice(k * n, (k + 1) * n)
            level = level + far[s, :n, cols] * far[s, :n, cols] + far[s, n:, cols] * far[s, n:, cols]
        live = (s < cnt_ref[0, 0]).astype(F32)
        misfit = live * (level - pat_ref[0, 0, s])
        for k in range(modes):
            for q in range(2):
                spot = (s, slice(q * n, (q + 1) * n), slice(k * n, (k + 1) * n))
                hi, lo = split(misfit * far[spot])
                yh[spot] = hi
                yl[spot] = lo

    def to_partner(p):
        return remote(term.at[p], tpart.at[p], t_send.at[0], t_recv.at[p], mate)

    def rows_of(owner, c):
        return pl.ds(pl.multiple_of(owner * slab + c * chunk, 8), chunk)

    def scatter(p, c, hop):
        return remote(
            acc.at[p, rows_of(hop_to(seat, hop), c)], pieces.at[p, c, hop - 1],
            rs_send.at[0], rs_recv.at[p, c], {"row": hop_to(me, hop)},
        )

    hops = list(range(1, group))
    for b in range(modes // 2):
        cols = slice(2 * b * n, 2 * (b + 1) * n)
        for s in range(slots):
            b_hi, b_lo = yh[s, :, cols], yl[s, :, cols]
            v = left3(r_hi[...], r_lo[...], b_hi, b_lo)
            for m in range(2):
                for q in range(2):
                    hi, lo = split(v[q * n : (q + 1) * n, m * n : (m + 1) * n])
                    vh[s, m * n : (m + 1) * n, q * n : (q + 1) * n] = hi
                    vl[s, m * n : (m + 1) * n, q * n : (q + 1) * n] = lo
        for m in range(2):
            k = 2 * b + m
            for s in range(slots):
                a_hi, a_lo = vh[s, m * n : (m + 1) * n, :], vl[s, m * n : (m + 1) * n, :]
                back = right3(a_hi, a_lo, l_hi[...], l_lo[...])
                br, bi = back[:, :n], back[:, n:]
                pr, pi = probe_ref[k, 0], probe_ref[k, 1]
                gr, gi = pr * br + pi * bi, pr * bi - pi * br
                wr, wi = win[s, 0], win[s, 1]
                tr, ti = wr * br + wi * bi, wr * bi - wi * br
                if k == 0:
                    gacc[s, 0], gacc[s, 1] = gr, gi
                else:
                    gacc[s, 0], gacc[s, 1] = gacc[s, 0] + gr, gacc[s, 1] + gi
                if s == 0:
                    term[k, :n], term[k, n:] = tr, ti
                else:
                    term[k, :n], term[k, n:] = term[k, :n] + tr, term[k, n:] + ti
            if k < pairs:
                to_partner(k).start()
            else:
                p = k - pairs
                with mark("w_partner"):
                    to_partner(p).wait_recv()
                acc[p] = term[k] + tpart[p]
                for c in range(CUTS):
                    for hop in hops:
                        scatter(p, c, hop).start()

    def across(j):
        return remote(gpar.at[j], grecv.at[j], g_send.at[0], g_recv.at[j], mate)

    for q in range(2):
        own = [jnp.zeros((n, n), F32)] * 3
        par = [jnp.zeros((n, n), F32)] * 3
        for s in range(slots):
            by, bx, sy, sx = place(s)
            g = pltpu.roll(pltpu.roll(gacc[s, q], sy, 0), sx, 1)
            low_x, low_y = (lane_id >= sx).astype(F32), (row_id >= sy).astype(F32)

            def side_of(block, at, low):
                return (block == at).astype(F32) * low + (block == at + 1).astype(F32) * (1.0 - low)

            g_own, g_par = g * side_of(1, bx, low_x), g * side_of(mine, bx, low_x)
            for j in range(3):
                mask = side_of(j, by, low_y)
                own[j] = own[j] + g_own * mask
                par[j] = par[j] + g_par * mask
        for j in range(3):
            gown[j, q * n : (q + 1) * n] = own[j]
            gpar[j, q * n : (q + 1) * n] = par[j]
    edge_far = remote(gown.at[far_at], gfar, e_send.at[0], e_recv.at[0], {"row": far_row})
    edge_via = remote(gown.at[far_at], gvia, e_send.at[0], e_recv.at[2], {"row": beyond})
    edge_near = remote(gown.at[near_at], gnear, e_send.at[1], e_recv.at[1], {"row": near})
    for j in (far_at, near_at, 1):
        across(j).start()
    with mark("w_across"):
        for j in (far_at, near_at):
            across(j).wait_recv()
            gown[j] = gown[j] + grecv[j]
        pl.when(passed)(edge_via.start)

    chunks = [(p, c) for p in range(pairs) for c in range(CUTS)]

    def exchange(r, p, c):
        return remote(
            part.at[p, c, r], swapped.at[p, c, r], x_send.at[0], x_recv.at[p, c, r], {"row": flip(me, ways[r])}
        )

    def gather(p, c, hop):
        here = fin.at[p, rows_of(seat, c)]
        return remote(here, here, ag_send.at[0], ag_recv.at[p, c], {"row": hop_to(me, hop)})

    def share(p, c, hop):
        at = rows_of(hop_to(seat, hop), c)
        return remote(fin.at[p, at], fin_other.at[p, at], o_send.at[0], o_recv.at[p], mate)

    def settle(r, p, c, total):
        if r < len(ways):
            part[p, c, r] = total
            exchange(r, p, c).start()
        else:
            fin[p, rows_of(seat, c)] = total
            for hop in hops:
                gather(p, c, hop).start()
            share(p, c, 0).start()

    def all_of(ref, send, recv):
        return remote(ref, ref, send, recv, mate)

    for p, c in chunks:
        total = acc[p, rows_of(seat, c)]
        with mark("w_rs"):
            all_of(pieces.at[p, c], rs_send.at[0], rs_recv.at[p, c]).wait_recv()
        for hop in hops:
            total = total + pieces[p, c, hop - 1]
        settle(0, p, c, total)
        if (p, c) == chunks[0]:
            pl.when(col == 0)(edge_near.start)
    pl.when(direct)(edge_far.start)

    with mark("w_via"):

        @pl.when(passes)
        def _():
            edge_via.wait_recv()
            gown[near_at] = gown[near_at] + gvia[...]

        pl.when(col == 1)(edge_near.start)
    for r in range(len(ways)):
        for p, c in chunks:
            with mark("w_xc"):
                exchange(r, p, c).wait_recv()
            settle(r + 1, p, c, part[p, c, r] + swapped[p, c, r])

    for p, c in chunks:
        with mark("w_ag"):
            all_of(pieces.at[p, c], ag_send.at[0], ag_recv.at[p, c]).wait_recv()
        for hop in hops:
            share(p, c, hop).start()
    for p in range(pairs):
        for q in range(2):
            half = slice(q * n, (q + 1) * n)
            probe_out[2 * p + col, q] = probe_ref[pairs + p, q] - probe_rate * fin[p, half] / tiles
    with mark("w_edge"):
        across(1).wait_recv()
        edge_near.wait_recv()
        pl.when(direct)(edge_far.wait_recv)
    for q in range(2):
        half = slice(q * n, (q + 1) * n)
        grad = gown[1, half] + grecv[1, half] + gnear[half] + gfar[half]
        obj_out[half] = frame[1, 1, half] - object_rate * grad / weight

    for p in range(pairs):
        with mark("w_share"):
            all_of(fin_other.at[p], o_send.at[0], o_recv.at[p]).wait_recv()
        for q in range(2):
            half = slice(q * n, (q + 1) * n)
            probe_out[2 * p + 1 - col, q] = probe_ref[p, q] - probe_rate * fin_other[p, half] / tiles

    with mark("w_sends"):
        to_mate.wait_send()
        to_near(0, whole).wait_send()
        pl.when(direct)(to_far(0, whole).wait_send)
        pl.when(passes)(pass_on(0, whole).wait_send)
        relay(near_at, 0, whole).wait_send()
        pl.when(has_far)(relay(far_at, 1, whole).wait_send)
        pl.when(has_far)(edge_far.wait_send)
        edge_near.wait_send()
        for ref, send, recv in (
            (tpart, t_send, t_recv.at[0]), (gpar, g_send, g_recv.at[0]), (pieces, rs_send, rs_recv.at[0, 0]),
            (pieces, ag_send, ag_recv.at[0, 0]), (fin_other, o_send, o_recv.at[0]),
        ):
            all_of(ref, send.at[0], recv).wait_send()
        if ways:
            all_of(part, x_send.at[0], x_recv.at[0, 0, 0]).wait_send()


def finish(obj_ref, probe_ref, obj_out, probe_out, sem):
    copies = [pltpu.make_async_copy(obj_ref, obj_out, sem.at[0])]
    for k in range(probe_ref.shape[0]):
        copies.append(pltpu.make_async_copy(probe_ref.at[k], probe_out.at[k], sem.at[k + 1]))
    for copy in copies:
        copy.start()
    for copy in copies:
        copy.wait()


def body(rows, object_field, probe, patterns, offsets, counts):
    modes, _, n, _ = probe.shape
    slots = patterns.shape[2]
    pairs = modes // 2
    assert rows > 1
    group, ways = plan(rows)
    block = object_field.reshape(2 * n, n)
    rounds = max(1, len(ways))
    chunk = 2 * n // group // CUTS
    tables = jnp.asarray(dft_tables(n))
    vmem = pl.BlockSpec(memory_space=pltpu.VMEM)
    hbm = pl.BlockSpec(memory_space=pltpu.HBM)
    dma = pltpu.SemaphoreType.DMA
    wide, tall = (slots, 2 * n, modes * n), (slots, modes * n, 2 * n)
    outs = (
        jax.ShapeDtypeStruct(block.shape, F32),
        jax.ShapeDtypeStruct(probe.shape, F32),
    )
    results = pl.pallas_call(
        functools.partial(kernel, rows, modes, slots, n),
        out_shape=outs,
        in_specs=[hbm] * 6,
        out_specs=(vmem, vmem),
        scratch_shapes=[
            pltpu.SMEM(offsets.shape, jnp.int32),
            pltpu.SMEM(counts.shape, jnp.int32),
            pltpu.VMEM(probe.shape, F32),
            pltpu.VMEM(patterns.shape, F32),
            pltpu.VMEM(tables.shape, BF16),
            pltpu.VMEM((3, 3, 2 * n, n), F32),
            pltpu.VMEM(tall, BF16),
            pltpu.VMEM(tall, BF16),
            pltpu.VMEM(wide, BF16),
            pltpu.VMEM(wide, BF16),
            pltpu.VMEM(wide, F32),
            pltpu.VMEM((slots, 2 * n, 2 * n), BF16),
            pltpu.VMEM((slots, 2 * n, 2 * n), BF16),
            pltpu.VMEM((slots, 2, n, n), F32),
            pltpu.VMEM((slots, 2, n, n), F32),
            pltpu.VMEM((3, 2 * n, n), F32),
            pltpu.VMEM((3, 2 * n, n), F32),
            pltpu.VMEM((3, 2 * n, n), F32),
            pltpu.VMEM((2 * n, n), F32),
            pltpu.VMEM((2 * n, n), F32),
            pltpu.VMEM((2 * n, n), F32),
            pltpu.VMEM((modes, 2 * n, n), F32),
            pltpu.VMEM((pairs, 2 * n, n), F32),
            pltpu.VMEM((pairs, 2 * n, n), F32),
            pltpu.VMEM((pairs, CUTS, group - 1, chunk, n), F32),
            pltpu.VMEM((pairs, CUTS, rounds, chunk, n), F32),
            pltpu.VMEM((pairs, CUTS, rounds, chunk, n), F32),
            pltpu.VMEM((pairs, 2 * n, n), F32),
            pltpu.VMEM((pairs, 2 * n, n), F32),
            dma((6,)),
            dma((1,)), dma((1,)),
            dma((1,)), dma((len(STRIPS),)),
            dma((1,)), dma((len(STRIPS),)), dma((1,)),
            dma((2,)), dma((2,)),
            dma((1,)), dma((3,)),
            dma((2,)), dma((3,)),
            dma((1,)), dma((pairs,)),
            dma((1,)), dma((pairs, CUTS)),
            dma((1,)), dma((pairs, CUTS, rounds)),
            dma((1,)), dma((pairs, CUTS)),
            dma((1,)), dma((pairs,)),
        ],
        compiler_params=pltpu.CompilerParams(
            collective_id=0, has_side_effects=True, vmem_limit_bytes=24 << 20
        ),
    )(*[pltpu.with_memory_space_constraint(x, pltpu.HBM) for x in (offsets,)], counts, *[pltpu.with_memory_space_constraint(x, pltpu.HBM) for x in (block, probe, patterns, tables)])
    new_block, new_probe = pl.pallas_call(
        finish,
        out_shape=outs,
        in_specs=[vmem] * 2,
        out_specs=(hbm, hbm),
        scratch_shapes=[dma((1 + modes,))],
        compiler_params=pltpu.CompilerParams(vmem_limit_bytes=4 << 20),
    )(*results)
    return new_block.reshape(object_field.shape), new_probe


def solution(mesh):
    placed = (
        P(None, ("tilt", "row"), "col"),
        P("tilt", None, None, None),
        P(("tilt", "row"), "col", None, None, None),
        P(("tilt", "row"), "col", None, None),
        P(("tilt", "row"), "col"),
    )
    return jax.shard_map(
        functools.partial(body, mesh.shape["row"]),
        mesh=mesh,
        in_specs=placed,
        out_specs=(P(None, ("tilt", "row"), "col"), P("tilt", None, None, None)),
        check_vma=False,
    )
```

```python
import contextlib
import functools

import jax
import jax.numpy as jnp
import numpy as np
from jax import lax
from jax.experimental import pallas as pl
from jax.experimental.pallas import tpu as pltpu
from jax.sharding import PartitionSpec as P

MESH = pl.DeviceIdType.MESH
F32 = jnp.float32
BF16 = jnp.bfloat16

object_rate = 1.0
probe_rate = 1.0
epsilon = 1e-06


def mark(name):
    return contextlib.nullcontext()


def split_table(table):
    high = table.astype(jnp.bfloat16)
    low = (table - high.astype(np.float64)).astype(jnp.bfloat16)
    return high, low


def dft_tables(length):
    counter = np.arange(length)
    product = counter[:, None] * counter[None, :] % length
    angle = -2.0 * np.pi / length * product
    c, s = np.cos(angle) / np.sqrt(length), np.sin(angle) / np.sqrt(length)
    right = np.block([[c, s], [-s, c]])
    left = right.T
    return np.stack([*split_table(right), *split_table(left)])


def split(x):
    high = x.astype(BF16)
    return high, (x - high.astype(F32)).astype(BF16)


def dot(a, b):
    return jnp.dot(a, b, preferred_element_type=F32)


def right3(a_hi, a_lo, hi, lo):
    m = a_hi.shape[0]
    both = dot(jnp.concatenate([a_hi, a_lo], 0), hi)
    return both[:m] + both[m:] + dot(a_hi, lo)


def left3(hi, lo, b_hi, b_lo):
    m = hi.shape[0]
    both = dot(jnp.concatenate([hi, lo], 0), b_hi)
    return both[:m] + both[m:] + dot(hi, b_lo)


def plan(rows):
    assert rows & (rows - 1) == 0
    group = min(4, rows)
    ways = []
    while group << len(ways) < rows:
        ways.append(group << len(ways))
    return group, ways


CUTS = 2
STRIPS = (2, 2, 2, 1, 1)


def kernel(
    rows, modes, slots, width,
    off_hbm, cnt_hbm, obj_hbm, probe_hbm, pat_hbm, tab_hbm,
    obj_out, probe_out,
    off_ref, cnt_ref, probe_ref, pat_ref, tab_ref,
    frame, xh, xl, yh, yl, far, vh, vl, win, gacc,
    gown, gpar, grecv, gnear, gfar, gvia, term, tpart, acc, pieces, part, swapped, fin, fin_other,
    load, hm_send, hm_recv, n_send, n_recv, f_send, f_recv, p_send, r_send, r_recv, g_send, g_recv,
    e_send, e_recv, t_send, t_recv, rs_send, rs_recv, x_send, x_recv, ag_send, ag_recv, o_send, o_recv, news,
):
    me = lax.axis_index("row")
    col = lax.axis_index("col")
    n = width
    tiles = rows * 2
    pairs = modes // 2
    group, ways = plan(rows)
    slab = 2 * n // group
    chunk = slab // CUTS
    mate = {"col": 1 - col}
    odd = lax.rem(me, 2)
    near_at, far_at = 2 - 2 * odd, 2 * odd
    near, far_row, beyond, behind = me + 1 - 2 * odd, me - 1 + 2 * odd, me - 2 + 4 * odd, me + 2 - 4 * odd
    has_far = jnp.logical_and(far_row >= 0, far_row < rows)
    direct = jnp.logical_and(has_far, col == 0)
    passes = jnp.logical_and(jnp.logical_and(behind >= 0, behind < rows), col == 1)
    passed = jnp.logical_and(has_far, col == 1)
    seat = lax.rem(me, group)

    def flip(index, bit):
        return jnp.where(lax.rem(index // bit, 2) == 0, index + bit, index - bit)

    def hop_to(index, hop):
        for b in range(hop.bit_length()):
            if hop >> b & 1:
                index = flip(index, 1 << b)
        return index

    def mode_at(spot):
        return 2 * spot + 1 - col if spot < pairs else 2 * (spot - pairs) + col

    obj_load = pltpu.make_async_copy(obj_hbm, frame.at[1, 1], load.at[0])
    loads = [
        pltpu.make_async_copy(off_hbm, off_ref, load.at[1]),
        pltpu.make_async_copy(cnt_hbm, cnt_ref, load.at[2]),
        pltpu.make_async_copy(pat_hbm, pat_ref, load.at[3]),
        pltpu.make_async_copy(tab_hbm, tab_ref, load.at[4]),
    ]
    probes = [pltpu.make_async_copy(probe_hbm.at[mode_at(j)], probe_ref.at[j], load.at[5]) for j in range(modes)]
    all_probes = pltpu.make_async_copy(probe_hbm, probe_ref, load.at[5])

    barrier = pltpu.get_barrier_semaphore()

    def greet(to):
        pl.semaphore_signal(barrier, inc=1, device_id=to, device_id_type=MESH)

    pl.when(has_far)(lambda: greet({"row": far_row}))
    greet({"row": near})
    greet(mate)
    for copy in [obj_load] + probes + loads:
        copy.start()
    with mark("w_barrier"):
        pl.semaphore_wait(barrier, 2 + has_far.astype(jnp.int32))

    rounds = [2]
    while 4 * rounds[-1] < rows:
        rounds.append(2 * rounds[-1])

    def sides(r):
        return (me - rounds[r], me - rounds[r] >= 0), (me + rounds[r], me + rounds[r] < rows)

    def tell(r):
        for row, there in sides(r):

            @pl.when(there)
            def _():
                pl.semaphore_signal(news.at[r], inc=1, device_id={"row": row}, device_id_type=MESH)

    def hear(r):
        (_, above), (_, below) = sides(r)
        pl.semaphore_wait(news.at[r], above.astype(jnp.int32) + below.astype(jnp.int32))

    def remote(src, dst, send, recv, to):
        return pltpu.make_async_remote_copy(
            src_ref=src, dst_ref=dst, send_sem=send, recv_sem=recv, device_id=to, device_id_type=MESH
        )

    seen = 2 * col
    mine = 2 - 2 * col
    unit = 2 * n // sum(STRIPS)
    starts = [unit * sum(STRIPS[:i]) for i in range(len(STRIPS) + 1)]
    strips = [pl.ds(starts[i], starts[i + 1] - starts[i]) for i in range(len(STRIPS))]
    to_mate = remote(obj_hbm, frame.at[1, seen], hm_send.at[0], hm_recv.at[0], mate)

    def to_near(i, at=None):
        at = strips[i] if at is None else at
        return remote(obj_hbm.at[at], frame.at[far_at, 1, at], n_send.at[0], n_recv.at[i], {"row": near})

    def to_far(i, at=None):
        at = strips[i] if at is None else at
        return remote(obj_hbm.at[at], frame.at[near_at, 1, at], f_send.at[0], f_recv.at[i], {"row": far_row})

    def pass_on(i, at=None):
        at = strips[i] if at is None else at
        return remote(
            frame.at[near_at, 1, at], frame.at[far_at, 1, at], p_send.at[0], f_recv.at[i], {"row": behind}
        )

    def relay(block, kind, at):
        return remote(
            frame.at[block, 1, at], frame.at[block, seen, at], r_send.at[kind], r_recv.at[kind], mate
        )

    whole = pl.ds(0, 2 * n)
    last = len(STRIPS)
    for i in range(last):
        to_near(i).start()
    for i in range(last):
        pl.when(direct)(to_far(i).start)
    to_mate.start()

    zero = jnp.zeros((2 * n, n), F32)
    for j in range(3):
        frame[j, seen] = zero

    @pl.when(jnp.logical_not(has_far))
    def _():
        frame[far_at, 1] = zero
        frame[far_at, mine] = zero

    @pl.when(jnp.logical_not(direct))
    def _():
        gfar[...] = zero

    with mark("w_load"):
        all_probes.wait()
    power = jnp.zeros((n, n), F32)
    for k in range(modes):
        power = power + (probe_ref[k, 0] * probe_ref[k, 0] + probe_ref[k, 1] * probe_ref[k, 1])
    weight = jnp.max(power) + epsilon

    with mark("w_halo"):
        def far_strip(i):
            @pl.when(has_far)
            def _():
                to_far(i).wait_recv()
                relay(far_at, 1, strips[i]).start()

        def near_strip(i):
            to_near(i).wait_recv()
            pl.when(passes)(pass_on(i).start)
            relay(near_at, 0, strips[i]).start()

        for i in range(last):
            near_strip(i)
        for i in range(last):
            far_strip(i)

    tell(0)
    obj_load.wait()
    for copy in loads:
        copy.wait()
    to_mate.wait_recv()
    with mark("w_relay"):
        relay(near_at, 0, whole).wait_recv()
        pl.when(has_far)(relay(far_at, 1, whole).wait_recv)

    r_hi, r_lo, l_hi, l_lo = (tab_ref.at[t] for t in range(4))
    row_id = lax.broadcasted_iota(jnp.int32, (n, n), 0)
    lane_id = lax.broadcasted_iota(jnp.int32, (n, n), 1)

    def place(s):
        oy, ox = off_ref[0, 0, s, 0], off_ref[0, 0, s, 1]
        by, bx = oy // n, ox // n
        return by, bx, oy - by * n, ox - bx * n

    for s in range(slots):
        by, bx, sy, sx = place(s)
        by2, bx2 = jnp.minimum(by + 1, 2), jnp.minimum(bx + 1, 2)
        for q in range(2):
            half = slice(q * n, (q + 1) * n)
            upper = jnp.where(lane_id >= sx, frame[by, bx, half], frame[by, bx2, half])
            lower = jnp.where(lane_id >= sx, frame[by2, bx, half], frame[by2, bx2, half])
            packed = jnp.where(row_id >= sy, upper, lower)
            packed = pltpu.roll(packed, lax.rem(n - sy, n), 0)
            win[s, q] = pltpu.roll(packed, lax.rem(n - sx, n), 1)
    for s in range(slots):
        for k in range(modes):
            wr, wi = win[s, 0], win[s, 1]
            pr, pi = probe_ref[k, 0], probe_ref[k, 1]
            for q, value in enumerate((pr * wr - pi * wi, pr * wi + pi * wr)):
                hi, lo = split(value)
                xh[s, k * n : (k + 1) * n, q * n : (q + 1) * n] = hi
                xl[s, k * n : (k + 1) * n, q * n : (q + 1) * n] = lo
    for s in range(slots):
        for k in range(modes):
            a_hi, a_lo = xh[s, k * n : (k + 1) * n, :], xl[s, k * n : (k + 1) * n, :]
            y = right3(a_hi, a_lo, r_hi[...], r_lo[...])
            for q in range(2):
                hi, lo = split(y[:, q * n : (q + 1) * n])
                yh[s, q * n : (q + 1) * n, k * n : (k + 1) * n] = hi
                yl[s, q * n : (q + 1) * n, k * n : (k + 1) * n] = lo
    for s in range(slots):
        for p in range(modes // 2):
            cols = slice(2 * p * n, 2 * (p + 1) * n)
            b_hi, b_lo = yh[s, :, cols], yl[s, :, cols]
            far[s, :, cols] = left3(l_hi[...], l_lo[...], b_hi, b_lo)
    for s in range(slots):
        level = jnp.zeros((n, n), F32)
        for k in range(modes):
            cols = slice(k * n, (k + 1) * n)
            level = level + far[s, :n, cols] * far[s, :n, cols] + far[s, n:, cols] * far[s, n:, cols]
        live = (s < cnt_ref[0, 0]).astype(F32)
        misfit = live * (level - pat_ref[0, 0, s])
        for k in range(modes):
            for q in range(2):
                spot = (s, slice(q * n, (q + 1) * n), slice(k * n, (k + 1) * n))
                hi, lo = split(misfit * far[spot])
                yh[spot] = hi
                yl[spot] = lo

    def to_partner(p):
        return remote(term.at[p], tpart.at[p], t_send.at[0], t_recv.at[p], mate)

    def rows_of(owner, c):
        return pl.ds(pl.multiple_of(owner * slab + c * chunk, 8), chunk)

    def scatter(p, c, hop):
        return remote(
            acc.at[p, rows_of(hop_to(seat, hop), c)], pieces.at[p, c, hop - 1],
            rs_send.at[0], rs_recv.at[p, c], {"row": hop_to(me, hop)},
        )

    hops = list(range(1, group))
    for b in range(modes // 2):
        cols = slice(2 * b * n, 2 * (b + 1) * n)
        for s in range(slots):
            b_hi, b_lo = yh[s, :, cols], yl[s, :, cols]
            v = left3(r_hi[...], r_lo[...], b_hi, b_lo)
            for m in range(2):
                for q in range(2):
                    hi, lo = split(v[q * n : (q + 1) * n, m * n : (m + 1) * n])
                    vh[s, m * n : (m + 1) * n, q * n : (q + 1) * n] = hi
                    vl[s, m * n : (m + 1) * n, q * n : (q + 1) * n] = lo
        for m in range(2):
            k = 2 * b + m
            for s in range(slots):
                a_hi, a_lo = vh[s, m * n : (m + 1) * n, :], vl[s, m * n : (m + 1) * n, :]
                back = right3(a_hi, a_lo, l_hi[...], l_lo[...])
                br, bi = back[:, :n], back[:, n:]
                pr, pi = probe_ref[k, 0], probe_ref[k, 1]
                gr, gi = pr * br + pi * bi, pr * bi - pi * br
                wr, wi = win[s, 0], win[s, 1]
                tr, ti = wr * br + wi * bi, wr * bi - wi * br
                if k == 0:
                    gacc[s, 0], gacc[s, 1] = gr, gi
                else:
                    gacc[s, 0], gacc[s, 1] = gacc[s, 0] + gr, gacc[s, 1] + gi
                if s == 0:
                    term[k, :n], term[k, n:] = tr, ti
                else:
                    term[k, :n], term[k, n:] = term[k, :n] + tr, term[k, n:] + ti
            if k < pairs:
                to_partner(k).start()
            else:
                p = k - pairs
                with mark("w_partner"):
                    to_partner(p).wait_recv()
                if p == 0:
                    for r in range(len(rounds)):
                        hear(r)
                        if r + 1 < len(rounds):
                            tell(r + 1)
                acc[p] = term[k] + tpart[p]
                for c in range(CUTS):
                    for hop in hops:
                        scatter(p, c, hop).start()

    def across(j):
        return remote(gpar.at[j], grecv.at[j], g_send.at[0], g_recv.at[j], mate)

    for q in range(2):
        own = [jnp.zeros((n, n), F32)] * 3
        par = [jnp.zeros((n, n), F32)] * 3
        for s in range(slots):
            by, bx, sy, sx = place(s)
            g = pltpu.roll(pltpu.roll(gacc[s, q], sy, 0), sx, 1)
            low_x, low_y = (lane_id >= sx).astype(F32), (row_id >= sy).astype(F32)

            def side_of(block, at, low):
                return (block == at).astype(F32) * low + (block == at + 1).astype(F32) * (1.0 - low)

            g_own, g_par = g * side_of(1, bx, low_x), g * side_of(mine, bx, low_x)
            for j in range(3):
                mask = side_of(j, by, low_y)
                own[j] = own[j] + g_own * mask
                par[j] = par[j] + g_par * mask
        for j in range(3):
            gown[j, q * n : (q + 1) * n] = own[j]
            gpar[j, q * n : (q + 1) * n] = par[j]
    edge_far = remote(gown.at[far_at], gfar, e_send.at[0], e_recv.at[0], {"row": far_row})
    edge_via = remote(gown.at[far_at], gvia, e_send.at[0], e_recv.at[2], {"row": beyond})
    edge_near = remote(gown.at[near_at], gnear, e_send.at[1], e_recv.at[1], {"row": near})
    for j in (far_at, near_at, 1):
        across(j).start()
    with mark("w_across"):
        for j in (far_at, near_at):
            across(j).wait_recv()
            gown[j] = gown[j] + grecv[j]
        pl.when(passed)(edge_via.start)

    chunks = [(p, c) for p in range(pairs) for c in range(CUTS)]

    def exchange(r, p, c):
        return remote(
            part.at[p, c, r], swapped.at[p, c, r], x_send.at[0], x_recv.at[p, c, r], {"row": flip(me, ways[r])}
        )

    def gather(p, c, hop):
        here = fin.at[p, rows_of(seat, c)]
        return remote(here, here, ag_send.at[0], ag_recv.at[p, c], {"row": hop_to(me, hop)})

    def share(p, c, hop):
        at = rows_of(hop_to(seat, hop), c)
        return remote(fin.at[p, at], fin_other.at[p, at], o_send.at[0], o_recv.at[p], mate)

    def settle(r, p, c, total):
        if r < len(ways):
            part[p, c, r] = total
            exchange(r, p, c).start()
        else:
            fin[p, rows_of(seat, c)] = total
            for hop in hops:
                gather(p, c, hop).start()
            share(p, c, 0).start()

    def all_of(ref, send, recv):
        return remote(ref, ref, send, recv, mate)

    for p, c in chunks:
        total = acc[p, rows_of(seat, c)]
        with mark("w_rs"):
            all_of(pieces.at[p, c], rs_send.at[0], rs_recv.at[p, c]).wait_recv()
        for hop in hops:
            total = total + pieces[p, c, hop - 1]
        settle(0, p, c, total)
        if (p, c) == chunks[0]:
            pl.when(col == 0)(edge_near.start)
    pl.when(direct)(edge_far.start)

    with mark("w_via"):

        @pl.when(passes)
        def _():
            edge_via.wait_recv()
            gown[near_at] = gown[near_at] + gvia[...]

        pl.when(col == 1)(edge_near.start)
    for r in range(len(ways)):
        for p, c in chunks:
            with mark("w_xc"):
                exchange(r, p, c).wait_recv()
            settle(r + 1, p, c, part[p, c, r] + swapped[p, c, r])

    for p, c in chunks:
        with mark("w_ag"):
            all_of(pieces.at[p, c], ag_send.at[0], ag_recv.at[p, c]).wait_recv()
        for hop in hops:
            share(p, c, hop).start()
    for p in range(pairs):
        for q in range(2):
            half = slice(q * n, (q + 1) * n)
            probe_out[2 * p + col, q] = probe_ref[pairs + p, q] - probe_rate * fin[p, half] / tiles
    with mark("w_edge"):
        across(1).wait_recv()
        edge_near.wait_recv()
        pl.when(direct)(edge_far.wait_recv)
    for q in range(2):
        half = slice(q * n, (q + 1) * n)
        grad = gown[1, half] + grecv[1, half] + gnear[half] + gfar[half]
        obj_out[half] = frame[1, 1, half] - object_rate * grad / weight

    for p in range(pairs):
        with mark("w_share"):
            all_of(fin_other.at[p], o_send.at[0], o_recv.at[p]).wait_recv()
        for q in range(2):
            half = slice(q * n, (q + 1) * n)
            probe_out[2 * p + 1 - col, q] = probe_ref[p, q] - probe_rate * fin_other[p, half] / tiles

    with mark("w_sends"):
        to_mate.wait_send()
        to_near(0, whole).wait_send()
        pl.when(direct)(to_far(0, whole).wait_send)
        pl.when(passes)(pass_on(0, whole).wait_send)
        relay(near_at, 0, whole).wait_send()
        pl.when(has_far)(relay(far_at, 1, whole).wait_send)
        pl.when(has_far)(edge_far.wait_send)
        edge_near.wait_send()
        for ref, send, recv in (
            (tpart, t_send, t_recv.at[0]), (gpar, g_send, g_recv.at[0]), (pieces, rs_send, rs_recv.at[0, 0]),
            (pieces, ag_send, ag_recv.at[0, 0]), (fin_other, o_send, o_recv.at[0]),
        ):
            all_of(ref, send.at[0], recv).wait_send()
        if ways:
            all_of(part, x_send.at[0], x_recv.at[0, 0, 0]).wait_send()


def finish(obj_ref, probe_ref, obj_out, probe_out, sem):
    copies = [pltpu.make_async_copy(obj_ref, obj_out, sem.at[0])]
    for k in range(probe_ref.shape[0]):
        copies.append(pltpu.make_async_copy(probe_ref.at[k], probe_out.at[k], sem.at[k + 1]))
    for copy in copies:
        copy.start()
    for copy in copies:
        copy.wait()


def body(rows, object_field, probe, patterns, offsets, counts):
    modes, _, n, _ = probe.shape
    slots = patterns.shape[2]
    pairs = modes // 2
    assert rows > 1
    group, ways = plan(rows)
    block = object_field.reshape(2 * n, n)
    rounds = max(1, len(ways))
    chunk = 2 * n // group // CUTS
    tables = jnp.asarray(dft_tables(n))
    vmem = pl.BlockSpec(memory_space=pltpu.VMEM)
    hbm = pl.BlockSpec(memory_space=pltpu.HBM)
    dma = pltpu.SemaphoreType.DMA
    wide, tall = (slots, 2 * n, modes * n), (slots, modes * n, 2 * n)
    outs = (
        jax.ShapeDtypeStruct(block.shape, F32),
        jax.ShapeDtypeStruct(probe.shape, F32),
    )
    results = pl.pallas_call(
        functools.partial(kernel, rows, modes, slots, n),
        out_shape=outs,
        in_specs=[hbm] * 6,
        out_specs=(vmem, vmem),
        scratch_shapes=[
            pltpu.SMEM(offsets.shape, jnp.int32),
            pltpu.SMEM(counts.shape, jnp.int32),
            pltpu.VMEM(probe.shape, F32),
            pltpu.VMEM(patterns.shape, F32),
            pltpu.VMEM(tables.shape, BF16),
            pltpu.VMEM((3, 3, 2 * n, n), F32),
            pltpu.VMEM(tall, BF16),
            pltpu.VMEM(tall, BF16),
            pltpu.VMEM(wide, BF16),
            pltpu.VMEM(wide, BF16),
            pltpu.VMEM(wide, F32),
            pltpu.VMEM((slots, 2 * n, 2 * n), BF16),
            pltpu.VMEM((slots, 2 * n, 2 * n), BF16),
            pltpu.VMEM((slots, 2, n, n), F32),
            pltpu.VMEM((slots, 2, n, n), F32),
            pltpu.VMEM((3, 2 * n, n), F32),
            pltpu.VMEM((3, 2 * n, n), F32),
            pltpu.VMEM((3, 2 * n, n), F32),
            pltpu.VMEM((2 * n, n), F32),
            pltpu.VMEM((2 * n, n), F32),
            pltpu.VMEM((2 * n, n), F32),
            pltpu.VMEM((modes, 2 * n, n), F32),
            pltpu.VMEM((pairs, 2 * n, n), F32),
            pltpu.VMEM((pairs, 2 * n, n), F32),
            pltpu.VMEM((pairs, CUTS, group - 1, chunk, n), F32),
            pltpu.VMEM((pairs, CUTS, rounds, chunk, n), F32),
            pltpu.VMEM((pairs, CUTS, rounds, chunk, n), F32),
            pltpu.VMEM((pairs, 2 * n, n), F32),
            pltpu.VMEM((pairs, 2 * n, n), F32),
            dma((6,)),
            dma((1,)), dma((1,)),
            dma((1,)), dma((len(STRIPS),)),
            dma((1,)), dma((len(STRIPS),)), dma((1,)),
            dma((2,)), dma((2,)),
            dma((1,)), dma((3,)),
            dma((2,)), dma((3,)),
            dma((1,)), dma((pairs,)),
            dma((1,)), dma((pairs, CUTS)),
            dma((1,)), dma((pairs, CUTS, rounds)),
            dma((1,)), dma((pairs, CUTS)),
            dma((1,)), dma((pairs,)),
            pltpu.SemaphoreType.REGULAR((rows.bit_length(),)),
        ],
        compiler_params=pltpu.CompilerParams(
            collective_id=0, has_side_effects=True, vmem_limit_bytes=24 << 20
        ),
    )(*[pltpu.with_memory_space_constraint(x, pltpu.HBM) for x in (offsets,)], counts, *[pltpu.with_memory_space_constraint(x, pltpu.HBM) for x in (block, probe, patterns, tables)])
    new_block, new_probe = pl.pallas_call(
        finish,
        out_shape=outs,
        in_specs=[vmem] * 2,
        out_specs=(hbm, hbm),
        scratch_shapes=[dma((1 + modes,))],
        compiler_params=pltpu.CompilerParams(vmem_limit_bytes=4 << 20),
    )(*results)
    return new_block.reshape(object_field.shape), new_probe


def solution(mesh):
    placed = (
        P(None, ("tilt", "row"), "col"),
        P("tilt", None, None, None),
        P(("tilt", "row"), "col", None, None, None),
        P(("tilt", "row"), "col", None, None),
        P(("tilt", "row"), "col"),
    )
    return jax.shard_map(
        functools.partial(body, mesh.shape["row"]),
        mesh=mesh,
        in_specs=placed,
        out_specs=(P(None, ("tilt", "row"), "col"), P("tilt", None, None, None)),
        check_vma=False,
    )
```

```python
import contextlib
import functools

import jax
import jax.numpy as jnp
import numpy as np
from jax import lax
from jax.experimental import pallas as pl
from jax.experimental.pallas import tpu as pltpu
from jax.sharding import PartitionSpec as P

MESH = pl.DeviceIdType.MESH
F32 = jnp.float32
BF16 = jnp.bfloat16

object_rate = 1.0
probe_rate = 1.0
epsilon = 1e-06


def mark(name):
    return contextlib.nullcontext()


def split_table(table):
    high = table.astype(jnp.bfloat16)
    low = (table - high.astype(np.float64)).astype(jnp.bfloat16)
    return high, low


def dft_tables(length):
    counter = np.arange(length)
    product = counter[:, None] * counter[None, :] % length
    angle = -2.0 * np.pi / length * product
    c, s = np.cos(angle) / np.sqrt(length), np.sin(angle) / np.sqrt(length)
    right = np.block([[c, s], [-s, c]])
    left = right.T
    return np.stack([*split_table(right), *split_table(left)])


def split(x):
    high = x.astype(BF16)
    return high, (x - high.astype(F32)).astype(BF16)


def dot(a, b):
    return jnp.dot(a, b, preferred_element_type=F32)


def right3(a_hi, a_lo, hi, lo):
    m = a_hi.shape[0]
    both = dot(jnp.concatenate([a_hi, a_lo], 0), hi)
    return both[:m] + both[m:] + dot(a_hi, lo)


def left3(hi, lo, b_hi, b_lo):
    m = hi.shape[0]
    both = dot(jnp.concatenate([hi, lo], 0), b_hi)
    return both[:m] + both[m:] + dot(hi, b_lo)


def plan(rows):
    assert rows & (rows - 1) == 0
    group = min(4, rows)
    ways = []
    while group << len(ways) < rows:
        ways.append(group << len(ways))
    return group, ways


def tells(rows):
    distances = [2]
    while 4 * distances[-1] < rows:
        distances.append(2 * distances[-1])
    return distances


CUTS = 2
STRIPS = (2, 2, 2, 1, 1)


def kernel(
    rows, modes, slots, width,
    off_hbm, cnt_hbm, obj_hbm, probe_hbm, pat_hbm, tab_hbm,
    obj_out, probe_out,
    off_ref, cnt_ref, probe_ref, pat_ref, tab_ref,
    frame, xh, xl, yh, yl, far, vh, vl, win, gacc,
    gown, gpar, grecv, gnear, gfar, gvia, tally, term, tpart, acc, pieces, part, swapped, fin, fin_other,
    load, sent, sent_far, sent_on, hm_recv, n_recv, f_recv, r_recv, g_recv,
    e_recv, t_recv, rs_recv, x_recv, ag_recv, o_recv, d_recv, news,
):
    me = lax.axis_index("row")
    col = lax.axis_index("col")
    n = width
    tiles = rows * 2
    pairs = modes // 2
    group, ways = plan(rows)
    slab = 2 * n // group
    chunk = slab // CUTS
    mate = {"col": 1 - col}
    odd = lax.rem(me, 2)
    near_at, far_at = 2 - 2 * odd, 2 * odd
    near, far_row, beyond, behind = me + 1 - 2 * odd, me - 1 + 2 * odd, me - 2 + 4 * odd, me + 2 - 4 * odd
    has_far = jnp.logical_and(far_row >= 0, far_row < rows)
    direct = jnp.logical_and(has_far, col == 0)
    passes = jnp.logical_and(jnp.logical_and(behind >= 0, behind < rows), col == 1)
    passed = jnp.logical_and(has_far, col == 1)
    seat = lax.rem(me, group)

    def flip(index, bit):
        return jnp.where(lax.rem(index // bit, 2) == 0, index + bit, index - bit)

    def hop_to(index, hop):
        for b in range(hop.bit_length()):
            if hop >> b & 1:
                index = flip(index, 1 << b)
        return index

    def mode_at(spot):
        return 2 * spot + 1 - col if spot < pairs else 2 * (spot - pairs) + col

    obj_load = pltpu.make_async_copy(obj_hbm, frame.at[1, 1], load.at[0])
    loads = [
        pltpu.make_async_copy(off_hbm, off_ref, load.at[1]),
        pltpu.make_async_copy(cnt_hbm, cnt_ref, load.at[2]),
    ]
    tables = pltpu.make_async_copy(tab_hbm, tab_ref, load.at[3])
    pattern = pltpu.make_async_copy(pat_hbm, pat_ref, load.at[4])
    probes = [pltpu.make_async_copy(probe_hbm.at[mode_at(j)], probe_ref.at[j], load.at[5]) for j in range(modes)]
    all_probes = pltpu.make_async_copy(probe_hbm, probe_ref, load.at[5])

    barrier = pltpu.get_barrier_semaphore()

    def greet(to):
        pl.semaphore_signal(barrier, inc=1, device_id=to, device_id_type=MESH)

    pl.when(has_far)(lambda: greet({"row": far_row}))
    greet({"row": near})
    greet(mate)
    for copy in [obj_load] + probes + loads + [tables, pattern]:
        copy.start()
    with mark("w_barrier"):
        pl.semaphore_wait(barrier, 2 + has_far.astype(jnp.int32))

    rounds = tells(rows)

    def sides(r):
        return (me - rounds[r], me - rounds[r] >= 0), (me + rounds[r], me + rounds[r] < rows)

    def tell(r):
        for row, there in sides(r):

            @pl.when(there)
            def _():
                pl.semaphore_signal(news.at[r], inc=1, device_id={"row": row}, device_id_type=MESH)

    def hear(r):
        (_, above), (_, below) = sides(r)
        pl.semaphore_wait(news.at[r], above.astype(jnp.int32) + below.astype(jnp.int32))

    def remote(src, dst, send, recv, to):
        return pltpu.make_async_remote_copy(
            src_ref=src, dst_ref=dst, send_sem=send, recv_sem=recv, device_id=to, device_id_type=MESH
        )

    seen = 2 * col
    mine = 2 - 2 * col
    unit = 2 * n // sum(STRIPS)
    starts = [unit * sum(STRIPS[:i]) for i in range(len(STRIPS) + 1)]
    strips = [pl.ds(starts[i], starts[i + 1] - starts[i]) for i in range(len(STRIPS))]
    to_mate = remote(obj_hbm, frame.at[1, seen], sent.at[0], hm_recv.at[0], mate)

    def to_near(i, at=None):
        at = strips[i] if at is None else at
        return remote(obj_hbm.at[at], frame.at[far_at, 1, at], sent.at[0], n_recv.at[i], {"row": near})

    def to_far(i, at=None):
        at = strips[i] if at is None else at
        return remote(obj_hbm.at[at], frame.at[near_at, 1, at], sent_on.at[0], f_recv.at[i], {"row": far_row})

    def pass_on(i, at=None):
        at = strips[i] if at is None else at
        return remote(
            frame.at[near_at, 1, at], frame.at[far_at, 1, at], sent_on.at[0], f_recv.at[i], {"row": behind}
        )

    def relay(block, kind, at):
        return remote(
            frame.at[block, 1, at], frame.at[block, seen, at], (sent, sent_far)[kind].at[0], r_recv.at[kind], mate
        )

    whole = pl.ds(0, 2 * n)
    last = len(STRIPS)
    for i in range(last):
        to_near(i).start()
    for i in range(last):
        pl.when(direct)(to_far(i).start)
    to_mate.start()

    zero = jnp.zeros((2 * n, n), F32)
    for j in range(3):
        frame[j, seen] = zero

    @pl.when(jnp.logical_not(has_far))
    def _():
        frame[far_at, 1] = zero
        frame[far_at, mine] = zero

    @pl.when(jnp.logical_not(direct))
    def _():
        gfar[...] = zero

    with mark("w_load"):
        all_probes.wait()
    power = jnp.zeros((n, n), F32)
    for k in range(modes):
        power = power + (probe_ref[k, 0] * probe_ref[k, 0] + probe_ref[k, 1] * probe_ref[k, 1])
    weight = jnp.max(power) + epsilon

    with mark("w_halo"):
        def far_strip(i):
            @pl.when(has_far)
            def _():
                to_far(i).wait_recv()
                relay(far_at, 1, strips[i]).start()

        def near_strip(i):
            to_near(i).wait_recv()
            pl.when(passes)(pass_on(i).start)
            relay(near_at, 0, strips[i]).start()

        for i in range(last):
            near_strip(i)
        for i in range(last):
            far_strip(i)

    tell(0)
    obj_load.wait()
    for copy in loads + [tables, pattern]:
        copy.wait()
    to_mate.wait_recv()
    with mark("w_relay"):
        relay(near_at, 0, whole).wait_recv()
        pl.when(has_far)(relay(far_at, 1, whole).wait_recv)

    r_hi, r_lo, l_hi, l_lo = (tab_ref.at[t] for t in range(4))
    row_id = lax.broadcasted_iota(jnp.int32, (n, n), 0)
    lane_id = lax.broadcasted_iota(jnp.int32, (n, n), 1)

    def place(s):
        oy, ox = off_ref[0, 0, s, 0], off_ref[0, 0, s, 1]
        by, bx = oy // n, ox // n
        return by, bx, oy - by * n, ox - bx * n

    for s in range(slots):
        by, bx, sy, sx = place(s)
        by2, bx2 = jnp.minimum(by + 1, 2), jnp.minimum(bx + 1, 2)
        for q in range(2):
            half = slice(q * n, (q + 1) * n)
            upper = jnp.where(lane_id >= sx, frame[by, bx, half], frame[by, bx2, half])
            lower = jnp.where(lane_id >= sx, frame[by2, bx, half], frame[by2, bx2, half])
            packed = jnp.where(row_id >= sy, upper, lower)
            packed = pltpu.roll(packed, lax.rem(n - sy, n), 0)
            win[s, q] = pltpu.roll(packed, lax.rem(n - sx, n), 1)
    for s in range(slots):
        for k in range(modes):
            wr, wi = win[s, 0], win[s, 1]
            pr, pi = probe_ref[k, 0], probe_ref[k, 1]
            for q, value in enumerate((pr * wr - pi * wi, pr * wi + pi * wr)):
                hi, lo = split(value)
                xh[s, k * n : (k + 1) * n, q * n : (q + 1) * n] = hi
                xl[s, k * n : (k + 1) * n, q * n : (q + 1) * n] = lo
    for s in range(slots):
        for k in range(modes):
            a_hi, a_lo = xh[s, k * n : (k + 1) * n, :], xl[s, k * n : (k + 1) * n, :]
            y = right3(a_hi, a_lo, r_hi[...], r_lo[...])
            for q in range(2):
                hi, lo = split(y[:, q * n : (q + 1) * n])
                yh[s, q * n : (q + 1) * n, k * n : (k + 1) * n] = hi
                yl[s, q * n : (q + 1) * n, k * n : (k + 1) * n] = lo
    for s in range(slots):
        for p in range(modes // 2):
            cols = slice(2 * p * n, 2 * (p + 1) * n)
            b_hi, b_lo = yh[s, :, cols], yl[s, :, cols]
            far[s, :, cols] = left3(l_hi[...], l_lo[...], b_hi, b_lo)
    for s in range(slots):
        level = jnp.zeros((n, n), F32)
        for k in range(modes):
            cols = slice(k * n, (k + 1) * n)
            level = level + far[s, :n, cols] * far[s, :n, cols] + far[s, n:, cols] * far[s, n:, cols]
        live = (s < cnt_ref[0, 0]).astype(F32)
        misfit = live * (level - pat_ref[0, 0, s])
        for k in range(modes):
            for q in range(2):
                spot = (s, slice(q * n, (q + 1) * n), slice(k * n, (k + 1) * n))
                hi, lo = split(misfit * far[spot])
                yh[spot] = hi
                yl[spot] = lo

    def to_partner(p):
        return remote(term.at[p], tpart.at[p], sent.at[0], t_recv.at[p], mate)

    def rows_of(owner, c):
        return pl.ds(pl.multiple_of(owner * slab + c * chunk, 8), chunk)

    def scatter(p, c, hop):
        return remote(
            acc.at[p, rows_of(hop_to(seat, hop), c)], pieces.at[p, c, hop - 1],
            sent.at[0], rs_recv.at[p, c], {"row": hop_to(me, hop)},
        )

    hops = list(range(1, group))
    for b in range(modes // 2):
        cols = slice(2 * b * n, 2 * (b + 1) * n)
        for s in range(slots):
            b_hi, b_lo = yh[s, :, cols], yl[s, :, cols]
            v = left3(r_hi[...], r_lo[...], b_hi, b_lo)
            for m in range(2):
                for q in range(2):
                    hi, lo = split(v[q * n : (q + 1) * n, m * n : (m + 1) * n])
                    vh[s, m * n : (m + 1) * n, q * n : (q + 1) * n] = hi
                    vl[s, m * n : (m + 1) * n, q * n : (q + 1) * n] = lo
        for m in range(2):
            k = 2 * b + m
            for s in range(slots):
                a_hi, a_lo = vh[s, m * n : (m + 1) * n, :], vl[s, m * n : (m + 1) * n, :]
                back = right3(a_hi, a_lo, l_hi[...], l_lo[...])
                br, bi = back[:, :n], back[:, n:]
                pr, pi = probe_ref[k, 0], probe_ref[k, 1]
                gr, gi = pr * br + pi * bi, pr * bi - pi * br
                wr, wi = win[s, 0], win[s, 1]
                tr, ti = wr * br + wi * bi, wr * bi - wi * br
                if k == 0:
                    gacc[s, 0], gacc[s, 1] = gr, gi
                else:
                    gacc[s, 0], gacc[s, 1] = gacc[s, 0] + gr, gacc[s, 1] + gi
                if s == 0:
                    term[k, :n], term[k, n:] = tr, ti
                else:
                    term[k, :n], term[k, n:] = term[k, :n] + tr, term[k, n:] + ti
            if k < pairs:
                to_partner(k).start()
            else:
                p = k - pairs
                with mark("w_partner"):
                    to_partner(p).wait_recv()
                if p == 0:
                    for r in range(len(rounds)):
                        hear(r)
                        if r + 1 < len(rounds):
                            tell(r + 1)
                acc[p] = term[k] + tpart[p]
                for c in range(CUTS):
                    for hop in hops:
                        scatter(p, c, hop).start()

    def across(j):
        return remote(gpar.at[j], grecv.at[j], sent.at[0], g_recv.at[j], mate)

    for q in range(2):
        own = [jnp.zeros((n, n), F32)] * 3
        par = [jnp.zeros((n, n), F32)] * 3
        for s in range(slots):
            by, bx, sy, sx = place(s)
            g = pltpu.roll(pltpu.roll(gacc[s, q], sy, 0), sx, 1)
            low_x, low_y = (lane_id >= sx).astype(F32), (row_id >= sy).astype(F32)

            def side_of(block, at, low):
                return (block == at).astype(F32) * low + (block == at + 1).astype(F32) * (1.0 - low)

            g_own, g_par = g * side_of(1, bx, low_x), g * side_of(mine, bx, low_x)
            for j in range(3):
                mask = side_of(j, by, low_y)
                own[j] = own[j] + g_own * mask
                par[j] = par[j] + g_par * mask
        for j in range(3):
            gown[j, q * n : (q + 1) * n] = own[j]
            gpar[j, q * n : (q + 1) * n] = par[j]
    edge_far = remote(gown.at[far_at], gfar, sent_far.at[0], e_recv.at[0], {"row": far_row})
    edge_via = remote(gown.at[far_at], gvia, sent_far.at[0], e_recv.at[2], {"row": beyond})
    edge_near = remote(gown.at[near_at], gnear, sent.at[0], e_recv.at[1], {"row": near})
    for j in (far_at, near_at, 1):
        across(j).start()
    with mark("w_across"):
        for j in (far_at, near_at):
            across(j).wait_recv()
            gown[j] = gown[j] + grecv[j]
        pl.when(passed)(edge_via.start)

    chunks = [(p, c) for p in range(pairs) for c in range(CUTS)]

    def exchange(r, p, c):
        return remote(
            part.at[p, c, r], swapped.at[p, c, r], sent.at[0], x_recv.at[p, c, r], {"row": flip(me, ways[r])}
        )

    def gather(p, c, hop):
        here = fin.at[p, rows_of(seat, c)]
        return remote(here, here, sent.at[0], ag_recv.at[p, c], {"row": hop_to(me, hop)})

    def gather_other(p, c, hop):
        return remote(
            fin.at[p, rows_of(seat, c)], fin_other.at[p, rows_of(seat, c)], sent.at[0], d_recv.at[0],
            {"row": hop_to(me, hop), "col": 1 - col},
        )

    def share(p, c, hop):
        at = rows_of(hop_to(seat, hop), c)
        return remote(fin.at[p, at], fin_other.at[p, at], sent.at[0], o_recv.at[p], mate)

    def settle(r, p, c, total):
        if r < len(ways):
            part[p, c, r] = total
            exchange(r, p, c).start()
        else:
            fin[p, rows_of(seat, c)] = total
            for hop in hops:
                gather(p, c, hop).start()
                if (p, c) == chunks[-1]:
                    gather_other(p, c, hop).start()
            share(p, c, 0).start()

    def all_of(ref, recv):
        return remote(ref, ref, sent.at[0], recv, mate)

    for p, c in chunks:
        total = acc[p, rows_of(seat, c)]
        with mark("w_rs"):
            all_of(pieces.at[p, c], rs_recv.at[p, c]).wait_recv()
        for hop in hops:
            total = total + pieces[p, c, hop - 1]
        settle(0, p, c, total)
        if (p, c) == chunks[0]:
            pl.when(col == 0)(edge_near.start)
    pl.when(direct)(edge_far.start)

    with mark("w_via"):

        @pl.when(passes)
        def _():
            edge_via.wait_recv()
            gown[near_at] = gown[near_at] + gvia[...]

        pl.when(col == 1)(edge_near.start)
    for r in range(len(ways)):
        for p, c in chunks:
            with mark("w_xc"):
                exchange(r, p, c).wait_recv()
            settle(r + 1, p, c, part[p, c, r] + swapped[p, c, r])

    for p, c in chunks:
        with mark("w_ag"):
            all_of(pieces.at[p, c], ag_recv.at[p, c]).wait_recv()
        for hop in hops:
            if (p, c) != chunks[-1]:
                share(p, c, hop).start()
    for p in range(pairs):
        for q in range(2):
            half = slice(q * n, (q + 1) * n)
            probe_out[2 * p + col, q] = probe_ref[pairs + p, q] - probe_rate * fin[p, half] / tiles
    with mark("w_edge"):
        across(1).wait_recv()
        edge_near.wait_recv()
        pl.when(direct)(edge_far.wait_recv)
    for q in range(2):
        half = slice(q * n, (q + 1) * n)
        grad = gown[1, half] + grecv[1, half] + gnear[half] + gfar[half]
        obj_out[half] = frame[1, 1, half] - object_rate * grad / weight

    for p in range(pairs):
        with mark("w_share"):
            if p < pairs - 1:
                all_of(fin_other.at[p], o_recv.at[p]).wait_recv()
            else:
                rest = pl.ds(0, 2 * n - (group - 1) * chunk)
                all_of(fin_other.at[p, rest], o_recv.at[p]).wait_recv()
                if hops:
                    all_of(pieces.at[0, 0], d_recv.at[0]).wait_recv()
        for q in range(2):
            half = slice(q * n, (q + 1) * n)
            probe_out[2 * p + 1 - col, q] = probe_ref[p, q] - probe_rate * fin_other[p, half] / tiles

    with mark("w_sends"):
        def drain(count, sem):
            here = tally.at[pl.ds(0, count)]
            remote(here, here, sem.at[0], hm_recv.at[0], mate).wait_send()

        drain(tally.shape[0], sent)
        pl.when(has_far)(lambda: drain(4 * n, sent_far))
        pl.when(jnp.logical_or(direct, passes))(lambda: drain(2 * n, sent_on))


def finish(obj_ref, probe_ref, obj_out, probe_out, sem):
    copies = [pltpu.make_async_copy(obj_ref, obj_out, sem.at[0])]
    for k in range(probe_ref.shape[0]):
        copies.append(pltpu.make_async_copy(probe_ref.at[k], probe_out.at[k], sem.at[k + 1]))
    for copy in copies:
        copy.start()
    for copy in copies:
        copy.wait()


def body(rows, object_field, probe, patterns, offsets, counts):
    modes, _, n, _ = probe.shape
    slots = patterns.shape[2]
    pairs = modes // 2
    assert rows > 1
    group, ways = plan(rows)
    block = object_field.reshape(2 * n, n)
    rounds = max(1, len(ways))
    chunk = 2 * n // group // CUTS
    rows_sent = 2 * n * (4 + pairs + 3 + pairs) + pairs * CUTS * chunk * (2 * (group - 1) + len(ways))
    tables = jnp.asarray(dft_tables(n))
    vmem = pl.BlockSpec(memory_space=pltpu.VMEM)
    hbm = pl.BlockSpec(memory_space=pltpu.HBM)
    dma = pltpu.SemaphoreType.DMA
    wide, tall = (slots, 2 * n, modes * n), (slots, modes * n, 2 * n)
    outs = (
        jax.ShapeDtypeStruct(block.shape, F32),
        jax.ShapeDtypeStruct(probe.shape, F32),
    )
    results = pl.pallas_call(
        functools.partial(kernel, rows, modes, slots, n),
        out_shape=outs,
        in_specs=[hbm] * 6,
        out_specs=(vmem, vmem),
        scratch_shapes=[
            pltpu.SMEM(offsets.shape, jnp.int32),
            pltpu.SMEM(counts.shape, jnp.int32),
            pltpu.VMEM(probe.shape, F32),
            pltpu.VMEM(patterns.shape, F32),
            pltpu.VMEM(tables.shape, BF16),
            pltpu.VMEM((3, 3, 2 * n, n), F32),
            pltpu.VMEM(tall, BF16),
            pltpu.VMEM(tall, BF16),
            pltpu.VMEM(wide, BF16),
            pltpu.VMEM(wide, BF16),
            pltpu.VMEM(wide, F32),
            pltpu.VMEM((slots, 2 * n, 2 * n), BF16),
            pltpu.VMEM((slots, 2 * n, 2 * n), BF16),
            pltpu.VMEM((slots, 2, n, n), F32),
            pltpu.VMEM((slots, 2, n, n), F32),
            pltpu.VMEM((3, 2 * n, n), F32),
            pltpu.VMEM((3, 2 * n, n), F32),
            pltpu.VMEM((3, 2 * n, n), F32),
            pltpu.VMEM((2 * n, n), F32),
            pltpu.VMEM((2 * n, n), F32),
            pltpu.VMEM((2 * n, n), F32),
            pltpu.VMEM((rows_sent, n), F32),
            pltpu.VMEM((modes, 2 * n, n), F32),
            pltpu.VMEM((pairs, 2 * n, n), F32),
            pltpu.VMEM((pairs, 2 * n, n), F32),
            pltpu.VMEM((pairs, CUTS, group - 1, chunk, n), F32),
            pltpu.VMEM((pairs, CUTS, rounds, chunk, n), F32),
            pltpu.VMEM((pairs, CUTS, rounds, chunk, n), F32),
            pltpu.VMEM((pairs, 2 * n, n), F32),
            pltpu.VMEM((pairs, 2 * n, n), F32),
            dma((6,)), dma((1,)), dma((1,)), dma((1,)),
            dma((1,)), dma((len(STRIPS),)), dma((len(STRIPS),)), dma((2,)), dma((3,)),
            dma((3,)), dma((pairs,)), dma((pairs, CUTS)), dma((pairs, CUTS, rounds)),
            dma((pairs, CUTS)), dma((pairs,)), dma((1,)),
            pltpu.SemaphoreType.REGULAR((len(tells(rows)),)),
        ],
        compiler_params=pltpu.CompilerParams(
            collective_id=0, has_side_effects=True, vmem_limit_bytes=24 << 20
        ),
    )(*[pltpu.with_memory_space_constraint(x, pltpu.HBM) for x in (offsets,)], counts, *[pltpu.with_memory_space_constraint(x, pltpu.HBM) for x in (block, probe, patterns, tables)])
    new_block, new_probe = pl.pallas_call(
        finish,
        out_shape=outs,
        in_specs=[vmem] * 2,
        out_specs=(hbm, hbm),
        scratch_shapes=[dma((1 + modes,))],
        compiler_params=pltpu.CompilerParams(vmem_limit_bytes=4 << 20),
    )(*results)
    return new_block.reshape(object_field.shape), new_probe


def solution(mesh):
    placed = (
        P(None, ("tilt", "row"), "col"),
        P("tilt", None, None, None),
        P(("tilt", "row"), "col", None, None, None),
        P(("tilt", "row"), "col", None, None),
        P(("tilt", "row"), "col"),
    )
    return jax.shard_map(
        functools.partial(body, mesh.shape["row"]),
        mesh=mesh,
        in_specs=placed,
        out_specs=(P(None, ("tilt", "row"), "col"), P("tilt", None, None, None)),
        check_vma=False,
    )
```

```python
import contextlib
import functools

import jax
import jax.numpy as jnp
import numpy as np
from jax import lax
from jax.experimental import pallas as pl
from jax.experimental.pallas import tpu as pltpu
from jax.sharding import PartitionSpec as P

MESH = pl.DeviceIdType.MESH
F32 = jnp.float32
BF16 = jnp.bfloat16

object_rate = 1.0
probe_rate = 1.0
epsilon = 1e-06


def mark(name):
    return contextlib.nullcontext()


def split_table(table):
    high = table.astype(jnp.bfloat16)
    low = (table - high.astype(np.float64)).astype(jnp.bfloat16)
    return high, low


def dft_tables(length):
    counter = np.arange(length)
    product = counter[:, None] * counter[None, :] % length
    angle = -2.0 * np.pi / length * product
    c, s = np.cos(angle) / np.sqrt(length), np.sin(angle) / np.sqrt(length)
    right = np.block([[c, s], [-s, c]])
    left = right.T
    return np.stack([*split_table(right), *split_table(left)])


def split(x):
    high = x.astype(BF16)
    return high, (x - high.astype(F32)).astype(BF16)


def dot(a, b):
    return jnp.dot(a, b, preferred_element_type=F32)


def right3(a_hi, a_lo, hi, lo):
    m = a_hi.shape[0]
    both = dot(jnp.concatenate([a_hi, a_lo], 0), hi)
    return both[:m] + both[m:] + dot(a_hi, lo)


def left3(hi, lo, b_hi, b_lo):
    m = hi.shape[0]
    both = dot(jnp.concatenate([hi, lo], 0), b_hi)
    return both[:m] + both[m:] + dot(hi, b_lo)


def plan(rows):
    assert rows & (rows - 1) == 0
    group = min(4, rows)
    ways = []
    while group << len(ways) < rows:
        ways.append(group << len(ways))
    return group, ways


def tells(rows):
    distances = [2]
    while 4 * distances[-1] < rows:
        distances.append(2 * distances[-1])
    return distances


CUTS = 2
STRIPS = (3, 3, 2)


def kernel(
    rows, modes, slots, width,
    off_hbm, cnt_hbm, obj_hbm, probe_hbm, pat_hbm, tab_hbm,
    obj_out, probe_out,
    off_ref, cnt_ref, probe_ref, pat_ref, tab_ref,
    frame, xh, xl, yh, yl, far, vh, vl, win, gacc,
    gown, gpar, grecv, gnear, gfar, gvia, tally, term, tpart, acc, pieces, part, swapped, fin, fin_other,
    load, sent, sent_far, sent_on, hm_recv, n_recv, f_recv, r_recv, g_recv,
    e_recv, t_recv, rs_recv, x_recv, ag_recv, o_recv, d_recv, news,
):
    me = lax.axis_index("row")
    col = lax.axis_index("col")
    n = width
    tiles = rows * 2
    pairs = modes // 2
    group, ways = plan(rows)
    slab = 2 * n // group
    chunk = slab // CUTS
    mate = {"col": 1 - col}
    odd = lax.rem(me, 2)
    near_at, far_at = 2 - 2 * odd, 2 * odd
    near, far_row, beyond, behind = me + 1 - 2 * odd, me - 1 + 2 * odd, me - 2 + 4 * odd, me + 2 - 4 * odd
    has_far = jnp.logical_and(far_row >= 0, far_row < rows)
    direct = jnp.logical_and(has_far, col == 0)
    passes = jnp.logical_and(jnp.logical_and(behind >= 0, behind < rows), col == 1)
    passed = jnp.logical_and(has_far, col == 1)
    seat = lax.rem(me, group)

    def flip(index, bit):
        return jnp.where(lax.rem(index // bit, 2) == 0, index + bit, index - bit)

    def hop_to(index, hop):
        for b in range(hop.bit_length()):
            if hop >> b & 1:
                index = flip(index, 1 << b)
        return index

    def mode_at(spot):
        return 2 * spot + 1 - col if spot < pairs else 2 * (spot - pairs) + col

    obj_load = pltpu.make_async_copy(obj_hbm, frame.at[1, 1], load.at[0])
    loads = [
        pltpu.make_async_copy(off_hbm, off_ref, load.at[1]),
        pltpu.make_async_copy(cnt_hbm, cnt_ref, load.at[2]),
    ]
    tables = pltpu.make_async_copy(tab_hbm, tab_ref, load.at[3])
    pattern = pltpu.make_async_copy(pat_hbm, pat_ref, load.at[4])
    probes = [pltpu.make_async_copy(probe_hbm.at[mode_at(j)], probe_ref.at[j], load.at[5]) for j in range(modes)]
    all_probes = pltpu.make_async_copy(probe_hbm, probe_ref, load.at[5])

    barrier = pltpu.get_barrier_semaphore()

    def greet(to):
        pl.semaphore_signal(barrier, inc=1, device_id=to, device_id_type=MESH)

    pl.when(has_far)(lambda: greet({"row": far_row}))
    greet({"row": near})
    greet(mate)
    for copy in [obj_load] + probes + loads + [tables, pattern]:
        copy.start()
    with mark("w_barrier"):
        pl.semaphore_wait(barrier, 2 + has_far.astype(jnp.int32))

    rounds = tells(rows)

    def sides(r):
        return (me - rounds[r], me - rounds[r] >= 0), (me + rounds[r], me + rounds[r] < rows)

    def tell(r):
        for row, there in sides(r):

            @pl.when(there)
            def _():
                pl.semaphore_signal(news.at[r], inc=1, device_id={"row": row}, device_id_type=MESH)

    def hear(r):
        (_, above), (_, below) = sides(r)
        pl.semaphore_wait(news.at[r], above.astype(jnp.int32) + below.astype(jnp.int32))

    def remote(src, dst, send, recv, to):
        return pltpu.make_async_remote_copy(
            src_ref=src, dst_ref=dst, send_sem=send, recv_sem=recv, device_id=to, device_id_type=MESH
        )

    seen = 2 * col
    mine = 2 - 2 * col
    unit = 2 * n // sum(STRIPS)
    starts = [unit * sum(STRIPS[:i]) for i in range(len(STRIPS) + 1)]
    strips = [pl.ds(starts[i], starts[i + 1] - starts[i]) for i in range(len(STRIPS))]
    to_mate = remote(obj_hbm, frame.at[1, seen], sent.at[0], hm_recv.at[0], mate)

    def to_near(i, at=None):
        at = strips[i] if at is None else at
        return remote(obj_hbm.at[at], frame.at[far_at, 1, at], sent.at[0], n_recv.at[i], {"row": near})

    def to_far(i, at=None):
        at = strips[i] if at is None else at
        return remote(obj_hbm.at[at], frame.at[near_at, 1, at], sent_on.at[0], f_recv.at[i], {"row": far_row})

    def pass_on(i, at=None):
        at = strips[i] if at is None else at
        return remote(
            frame.at[near_at, 1, at], frame.at[far_at, 1, at], sent_on.at[0], f_recv.at[i], {"row": behind}
        )

    def relay(block, kind, at):
        return remote(
            frame.at[block, 1, at], frame.at[block, seen, at], (sent, sent_far)[kind].at[0], r_recv.at[kind], mate
        )

    whole = pl.ds(0, 2 * n)
    last = len(STRIPS)
    for i in range(last):
        to_near(i).start()
    for i in range(last):
        pl.when(direct)(to_far(i).start)
    to_mate.start()

    zero = jnp.zeros((2 * n, n), F32)
    for j in range(3):
        frame[j, seen] = zero

    @pl.when(jnp.logical_not(has_far))
    def _():
        frame[far_at, 1] = zero
        frame[far_at, mine] = zero

    @pl.when(jnp.logical_not(direct))
    def _():
        gfar[...] = zero

    with mark("w_load"):
        all_probes.wait()
    power = jnp.zeros((n, n), F32)
    for k in range(modes):
        power = power + (probe_ref[k, 0] * probe_ref[k, 0] + probe_ref[k, 1] * probe_ref[k, 1])
    weight = jnp.max(power) + epsilon

    with mark("w_halo"):
        def far_strip(i):
            @pl.when(has_far)
            def _():
                to_far(i).wait_recv()
                relay(far_at, 1, strips[i]).start()

        def near_strip(i):
            to_near(i).wait_recv()
            pl.when(passes)(pass_on(i).start)
            relay(near_at, 0, strips[i]).start()

        for i in range(last):
            near_strip(i)
        for i in range(last):
            far_strip(i)

    tell(0)
    obj_load.wait()
    for copy in loads + [tables, pattern]:
        copy.wait()
    to_mate.wait_recv()
    with mark("w_relay"):
        relay(near_at, 0, whole).wait_recv()
        pl.when(has_far)(relay(far_at, 1, whole).wait_recv)

    r_hi, r_lo, l_hi, l_lo = (tab_ref.at[t] for t in range(4))
    row_id = lax.broadcasted_iota(jnp.int32, (n, n), 0)
    lane_id = lax.broadcasted_iota(jnp.int32, (n, n), 1)

    def place(s):
        oy, ox = off_ref[0, 0, s, 0], off_ref[0, 0, s, 1]
        by, bx = oy // n, ox // n
        return by, bx, oy - by * n, ox - bx * n

    for s in range(slots):
        by, bx, sy, sx = place(s)
        by2, bx2 = jnp.minimum(by + 1, 2), jnp.minimum(bx + 1, 2)
        for q in range(2):
            half = slice(q * n, (q + 1) * n)
            upper = jnp.where(lane_id >= sx, frame[by, bx, half], frame[by, bx2, half])
            lower = jnp.where(lane_id >= sx, frame[by2, bx, half], frame[by2, bx2, half])
            packed = jnp.where(row_id >= sy, upper, lower)
            packed = pltpu.roll(packed, lax.rem(n - sy, n), 0)
            win[s, q] = pltpu.roll(packed, lax.rem(n - sx, n), 1)
    for s in range(slots):
        for k in range(modes):
            wr, wi = win[s, 0], win[s, 1]
            pr, pi = probe_ref[k, 0], probe_ref[k, 1]
            for q, value in enumerate((pr * wr - pi * wi, pr * wi + pi * wr)):
                hi, lo = split(value)
                xh[s, k * n : (k + 1) * n, q * n : (q + 1) * n] = hi
                xl[s, k * n : (k + 1) * n, q * n : (q + 1) * n] = lo
    for s in range(slots):
        for k in range(modes):
            a_hi, a_lo = xh[s, k * n : (k + 1) * n, :], xl[s, k * n : (k + 1) * n, :]
            y = right3(a_hi, a_lo, r_hi[...], r_lo[...])
            for q in range(2):
                hi, lo = split(y[:, q * n : (q + 1) * n])
                yh[s, q * n : (q + 1) * n, k * n : (k + 1) * n] = hi
                yl[s, q * n : (q + 1) * n, k * n : (k + 1) * n] = lo
    for s in range(slots):
        for p in range(modes // 2):
            cols = slice(2 * p * n, 2 * (p + 1) * n)
            b_hi, b_lo = yh[s, :, cols], yl[s, :, cols]
            far[s, :, cols] = left3(l_hi[...], l_lo[...], b_hi, b_lo)
    for s in range(slots):
        level = jnp.zeros((n, n), F32)
        for k in range(modes):
            cols = slice(k * n, (k + 1) * n)
            level = level + far[s, :n, cols] * far[s, :n, cols] + far[s, n:, cols] * far[s, n:, cols]
        live = (s < cnt_ref[0, 0]).astype(F32)
        misfit = live * (level - pat_ref[0, 0, s])
        for k in range(modes):
            for q in range(2):
                spot = (s, slice(q * n, (q + 1) * n), slice(k * n, (k + 1) * n))
                hi, lo = split(misfit * far[spot])
                yh[spot] = hi
                yl[spot] = lo

    def to_partner(p):
        return remote(term.at[p], tpart.at[p], sent.at[0], t_recv.at[p], mate)

    def rows_of(owner, c):
        return pl.ds(pl.multiple_of(owner * slab + c * chunk, 8), chunk)

    def scatter(p, c, hop):
        return remote(
            acc.at[p, rows_of(hop_to(seat, hop), c)], pieces.at[p, c, hop - 1],
            sent.at[0], rs_recv.at[p, c], {"row": hop_to(me, hop)},
        )

    hops = list(range(1, group))
    for b in range(modes // 2):
        cols = slice(2 * b * n, 2 * (b + 1) * n)
        for s in range(slots):
            b_hi, b_lo = yh[s, :, cols], yl[s, :, cols]
            v = left3(r_hi[...], r_lo[...], b_hi, b_lo)
            for m in range(2):
                for q in range(2):
                    hi, lo = split(v[q * n : (q + 1) * n, m * n : (m + 1) * n])
                    vh[s, m * n : (m + 1) * n, q * n : (q + 1) * n] = hi
                    vl[s, m * n : (m + 1) * n, q * n : (q + 1) * n] = lo
        for m in range(2):
            k = 2 * b + m
            for s in range(slots):
                a_hi, a_lo = vh[s, m * n : (m + 1) * n, :], vl[s, m * n : (m + 1) * n, :]
                back = right3(a_hi, a_lo, l_hi[...], l_lo[...])
                br, bi = back[:, :n], back[:, n:]
                pr, pi = probe_ref[k, 0], probe_ref[k, 1]
                gr, gi = pr * br + pi * bi, pr * bi - pi * br
                wr, wi = win[s, 0], win[s, 1]
                tr, ti = wr * br + wi * bi, wr * bi - wi * br
                if k == 0:
                    gacc[s, 0], gacc[s, 1] = gr, gi
                else:
                    gacc[s, 0], gacc[s, 1] = gacc[s, 0] + gr, gacc[s, 1] + gi
                if s == 0:
                    term[k, :n], term[k, n:] = tr, ti
                else:
                    term[k, :n], term[k, n:] = term[k, :n] + tr, term[k, n:] + ti
            if k < pairs:
                to_partner(k).start()
            else:
                p = k - pairs
                with mark("w_partner"):
                    to_partner(p).wait_recv()
                if p == 0:
                    for r in range(len(rounds)):
                        hear(r)
                        if r + 1 < len(rounds):
                            tell(r + 1)
                acc[p] = term[k] + tpart[p]
                for c in range(CUTS):
                    for hop in hops[::-1]:
                        scatter(p, c, hop).start()

    def across(j):
        return remote(gpar.at[j], grecv.at[j], sent.at[0], g_recv.at[j], mate)

    for q in range(2):
        own = [jnp.zeros((n, n), F32)] * 3
        par = [jnp.zeros((n, n), F32)] * 3
        for s in range(slots):
            by, bx, sy, sx = place(s)
            g = pltpu.roll(pltpu.roll(gacc[s, q], sy, 0), sx, 1)
            low_x, low_y = (lane_id >= sx).astype(F32), (row_id >= sy).astype(F32)

            def side_of(block, at, low):
                return (block == at).astype(F32) * low + (block == at + 1).astype(F32) * (1.0 - low)

            g_own, g_par = g * side_of(1, bx, low_x), g * side_of(mine, bx, low_x)
            for j in range(3):
                mask = side_of(j, by, low_y)
                own[j] = own[j] + g_own * mask
                par[j] = par[j] + g_par * mask
        for j in range(3):
            gown[j, q * n : (q + 1) * n] = own[j]
            gpar[j, q * n : (q + 1) * n] = par[j]
    edge_far = remote(gown.at[far_at], gfar, sent_far.at[0], e_recv.at[0], {"row": far_row})
    edge_via = remote(gown.at[far_at], gvia, sent_far.at[0], e_recv.at[2], {"row": beyond})
    edge_near = remote(gown.at[near_at], gnear, sent.at[0], e_recv.at[1], {"row": near})
    for j in (far_at, near_at, 1):
        across(j).start()
    with mark("w_across"):
        for j in (far_at, near_at):
            across(j).wait_recv()
            gown[j] = gown[j] + grecv[j]
        pl.when(passed)(edge_via.start)

    chunks = [(p, c) for p in range(pairs) for c in range(CUTS)]

    def exchange(r, p, c):
        return remote(
            part.at[p, c, r], swapped.at[p, c, r], sent.at[0], x_recv.at[p, c, r], {"row": flip(me, ways[r])}
        )

    def gather(p, c, hop):
        here = fin.at[p, rows_of(seat, c)]
        return remote(here, here, sent.at[0], ag_recv.at[p, c], {"row": hop_to(me, hop)})

    def gather_other(p, c, hop):
        return remote(
            fin.at[p, rows_of(seat, c)], fin_other.at[p, rows_of(seat, c)], sent.at[0], d_recv.at[0],
            {"row": hop_to(me, hop), "col": 1 - col},
        )

    def share(p, c, hop):
        at = rows_of(hop_to(seat, hop), c)
        return remote(fin.at[p, at], fin_other.at[p, at], sent.at[0], o_recv.at[p], mate)

    def settle(r, p, c, total):
        if r < len(ways):
            part[p, c, r] = total
            exchange(r, p, c).start()
        else:
            fin[p, rows_of(seat, c)] = total
            for hop in hops:
                gather(p, c, hop).start()
                if (p, c) == chunks[-1]:
                    gather_other(p, c, hop).start()
            share(p, c, 0).start()

    def all_of(ref, recv):
        return remote(ref, ref, sent.at[0], recv, mate)

    for p, c in chunks:
        total = acc[p, rows_of(seat, c)]
        with mark("w_rs"):
            all_of(pieces.at[p, c], rs_recv.at[p, c]).wait_recv()
        for hop in hops:
            total = total + pieces[p, c, hop - 1]
        settle(0, p, c, total)
        if (p, c) == chunks[0]:
            pl.when(col == 0)(edge_near.start)
    pl.when(direct)(edge_far.start)

    with mark("w_via"):

        @pl.when(passes)
        def _():
            edge_via.wait_recv()
            gown[near_at] = gown[near_at] + gvia[...]

        pl.when(col == 1)(edge_near.start)
    for r in range(len(ways)):
        for p, c in chunks:
            with mark("w_xc"):
                exchange(r, p, c).wait_recv()
            settle(r + 1, p, c, part[p, c, r] + swapped[p, c, r])

    for p, c in chunks:
        with mark("w_ag"):
            all_of(pieces.at[p, c], ag_recv.at[p, c]).wait_recv()
        for hop in hops:
            if (p, c) != chunks[-1]:
                share(p, c, hop).start()
    for p in range(pairs):
        for q in range(2):
            half = slice(q * n, (q + 1) * n)
            probe_out[2 * p + col, q] = probe_ref[pairs + p, q] - probe_rate * fin[p, half] / tiles
    with mark("w_edge"):
        across(1).wait_recv()
        edge_near.wait_recv()
        pl.when(direct)(edge_far.wait_recv)
    for q in range(2):
        half = slice(q * n, (q + 1) * n)
        grad = gown[1, half] + grecv[1, half] + gnear[half] + gfar[half]
        obj_out[half] = frame[1, 1, half] - object_rate * grad / weight

    for p in range(pairs):
        with mark("w_share"):
            if p < pairs - 1:
                all_of(fin_other.at[p], o_recv.at[p]).wait_recv()
            else:
                rest = pl.ds(0, 2 * n - (group - 1) * chunk)
                all_of(fin_other.at[p, rest], o_recv.at[p]).wait_recv()
                if hops:
                    all_of(pieces.at[0, 0], d_recv.at[0]).wait_recv()
        for q in range(2):
            half = slice(q * n, (q + 1) * n)
            probe_out[2 * p + 1 - col, q] = probe_ref[p, q] - probe_rate * fin_other[p, half] / tiles

    with mark("w_sends"):
        def drain(count, sem):
            here = tally.at[pl.ds(0, count)]
            remote(here, here, sem.at[0], hm_recv.at[0], mate).wait_send()

        drain(tally.shape[0], sent)
        pl.when(has_far)(lambda: drain(4 * n, sent_far))
        pl.when(jnp.logical_or(direct, passes))(lambda: drain(2 * n, sent_on))


def finish(obj_ref, probe_ref, obj_out, probe_out, sem):
    copies = [pltpu.make_async_copy(obj_ref, obj_out, sem.at[0])]
    for k in range(probe_ref.shape[0]):
        copies.append(pltpu.make_async_copy(probe_ref.at[k], probe_out.at[k], sem.at[k + 1]))
    for copy in copies:
        copy.start()
    for copy in copies:
        copy.wait()


def body(rows, object_field, probe, patterns, offsets, counts):
    modes, _, n, _ = probe.shape
    slots = patterns.shape[2]
    pairs = modes // 2
    assert rows > 1
    group, ways = plan(rows)
    block = object_field.reshape(2 * n, n)
    rounds = max(1, len(ways))
    chunk = 2 * n // group // CUTS
    rows_sent = 2 * n * (4 + pairs + 3 + pairs) + pairs * CUTS * chunk * (2 * (group - 1) + len(ways))
    tables = jnp.asarray(dft_tables(n))
    vmem = pl.BlockSpec(memory_space=pltpu.VMEM)
    hbm = pl.BlockSpec(memory_space=pltpu.HBM)
    dma = pltpu.SemaphoreType.DMA
    wide, tall = (slots, 2 * n, modes * n), (slots, modes * n, 2 * n)
    outs = (
        jax.ShapeDtypeStruct(block.shape, F32),
        jax.ShapeDtypeStruct(probe.shape, F32),
    )
    results = pl.pallas_call(
        functools.partial(kernel, rows, modes, slots, n),
        out_shape=outs,
        in_specs=[hbm] * 6,
        out_specs=(vmem, vmem),
        scratch_shapes=[
            pltpu.SMEM(offsets.shape, jnp.int32),
            pltpu.SMEM(counts.shape, jnp.int32),
            pltpu.VMEM(probe.shape, F32),
            pltpu.VMEM(patterns.shape, F32),
            pltpu.VMEM(tables.shape, BF16),
            pltpu.VMEM((3, 3, 2 * n, n), F32),
            pltpu.VMEM(tall, BF16),
            pltpu.VMEM(tall, BF16),
            pltpu.VMEM(wide, BF16),
            pltpu.VMEM(wide, BF16),
            pltpu.VMEM(wide, F32),
            pltpu.VMEM((slots, 2 * n, 2 * n), BF16),
            pltpu.VMEM((slots, 2 * n, 2 * n), BF16),
            pltpu.VMEM((slots, 2, n, n), F32),
            pltpu.VMEM((slots, 2, n, n), F32),
            pltpu.VMEM((3, 2 * n, n), F32),
            pltpu.VMEM((3, 2 * n, n), F32),
            pltpu.VMEM((3, 2 * n, n), F32),
            pltpu.VMEM((2 * n, n), F32),
            pltpu.VMEM((2 * n, n), F32),
            pltpu.VMEM((2 * n, n), F32),
            pltpu.VMEM((rows_sent, n), F32),
            pltpu.VMEM((modes, 2 * n, n), F32),
            pltpu.VMEM((pairs, 2 * n, n), F32),
            pltpu.VMEM((pairs, 2 * n, n), F32),
            pltpu.VMEM((pairs, CUTS, group - 1, chunk, n), F32),
            pltpu.VMEM((pairs, CUTS, rounds, chunk, n), F32),
            pltpu.VMEM((pairs, CUTS, rounds, chunk, n), F32),
            pltpu.VMEM((pairs, 2 * n, n), F32),
            pltpu.VMEM((pairs, 2 * n, n), F32),
            dma((6,)), dma((1,)), dma((1,)), dma((1,)),
            dma((1,)), dma((len(STRIPS),)), dma((len(STRIPS),)), dma((2,)), dma((3,)),
            dma((3,)), dma((pairs,)), dma((pairs, CUTS)), dma((pairs, CUTS, rounds)),
            dma((pairs, CUTS)), dma((pairs,)), dma((1,)),
            pltpu.SemaphoreType.REGULAR((len(tells(rows)),)),
        ],
        compiler_params=pltpu.CompilerParams(
            collective_id=0, has_side_effects=True, vmem_limit_bytes=24 << 20
        ),
    )(*[pltpu.with_memory_space_constraint(x, pltpu.HBM) for x in (offsets,)], counts, *[pltpu.with_memory_space_constraint(x, pltpu.HBM) for x in (block, probe, patterns, tables)])
    new_block, new_probe = pl.pallas_call(
        finish,
        out_shape=outs,
        in_specs=[vmem] * 2,
        out_specs=(hbm, hbm),
        scratch_shapes=[dma((1 + modes,))],
        compiler_params=pltpu.CompilerParams(vmem_limit_bytes=4 << 20),
    )(*results)
    return new_block.reshape(object_field.shape), new_probe


def solution(mesh):
    placed = (
        P(None, ("tilt", "row"), "col"),
        P("tilt", None, None, None),
        P(("tilt", "row"), "col", None, None, None),
        P(("tilt", "row"), "col", None, None),
        P(("tilt", "row"), "col"),
    )
    return jax.shard_map(
        functools.partial(body, mesh.shape["row"]),
        mesh=mesh,
        in_specs=placed,
        out_specs=(P(None, ("tilt", "row"), "col"), P("tilt", None, None, None)),
        check_vma=False,
    )
```

```python
import contextlib
import functools

import jax
import jax.numpy as jnp
import numpy as np
from jax import lax
from jax.experimental import pallas as pl
from jax.experimental.pallas import tpu as pltpu
from jax.sharding import PartitionSpec as P

MESH = pl.DeviceIdType.MESH
F32 = jnp.float32
BF16 = jnp.bfloat16

object_rate = 1.0
probe_rate = 1.0
epsilon = 1e-06


def mark(name):
    return contextlib.nullcontext()


def split_table(table):
    high = table.astype(jnp.bfloat16)
    low = (table - high.astype(np.float64)).astype(jnp.bfloat16)
    return high, low


def dft_tables(length):
    counter = np.arange(length)
    product = counter[:, None] * counter[None, :] % length
    angle = -2.0 * np.pi / length * product
    c, s = np.cos(angle) / np.sqrt(length), np.sin(angle) / np.sqrt(length)
    right = np.block([[c, s], [-s, c]])
    left = right.T
    return np.stack([*split_table(right), *split_table(left)])


def split(x):
    high = x.astype(BF16)
    return high, (x - high.astype(F32)).astype(BF16)


def dot(a, b):
    return jnp.dot(a, b, preferred_element_type=F32)


def right3(a_hi, a_lo, hi, lo):
    m = a_hi.shape[0]
    both = dot(jnp.concatenate([a_hi, a_lo], 0), hi)
    return both[:m] + both[m:] + dot(a_hi, lo)


def left3(hi, lo, b_hi, b_lo):
    m = hi.shape[0]
    both = dot(jnp.concatenate([hi, lo], 0), b_hi)
    return both[:m] + both[m:] + dot(hi, b_lo)


def plan(rows):
    assert rows & (rows - 1) == 0
    group = min(4, rows)
    ways = []
    while group << len(ways) < rows:
        ways.append(group << len(ways))
    return group, ways


def tells(rows):
    distances = [2]
    while 4 * distances[-1] < rows:
        distances.append(2 * distances[-1])
    return distances


CUTS = 2
STRIPS = (3, 3, 2)


def kernel(
    rows, modes, slots, width,
    off_hbm, cnt_hbm, obj_hbm, probe_hbm, pat_hbm, tab_hbm,
    obj_out, probe_out,
    off_ref, cnt_ref, probe_ref, pat_ref, tab_ref,
    frame, xh, xl, yh, yl, far, vh, vl, win, gacc,
    gown, gpar, grecv, gnear, gfar, gvia, tally, term, tpart, acc, pieces, part, swapped, fin, fin_other,
    load, sent, sent_far, sent_on, hm_recv, n_recv, f_recv, r_recv, g_recv,
    e_recv, t_recv, rs_recv, x_recv, ag_recv, o_recv, news,
):
    me = lax.axis_index("row")
    col = lax.axis_index("col")
    n = width
    tiles = rows * 2
    pairs = modes // 2
    group, ways = plan(rows)
    slab = 2 * n // group
    chunk = slab // CUTS
    mate = {"col": 1 - col}
    odd = lax.rem(me, 2)
    near_at, far_at = 2 - 2 * odd, 2 * odd
    near, far_row, beyond, behind = me + 1 - 2 * odd, me - 1 + 2 * odd, me - 2 + 4 * odd, me + 2 - 4 * odd
    has_far = jnp.logical_and(far_row >= 0, far_row < rows)
    direct = jnp.logical_and(has_far, col == 0)
    passes = jnp.logical_and(jnp.logical_and(behind >= 0, behind < rows), col == 1)
    passed = jnp.logical_and(has_far, col == 1)
    seat = lax.rem(me, group)

    def flip(index, bit):
        return jnp.where(lax.rem(index // bit, 2) == 0, index + bit, index - bit)

    def hop_to(index, hop):
        for b in range(hop.bit_length()):
            if hop >> b & 1:
                index = flip(index, 1 << b)
        return index

    def mode_at(spot):
        return 2 * spot + 1 - col if spot < pairs else 2 * (spot - pairs) + col

    obj_load = pltpu.make_async_copy(obj_hbm, frame.at[1, 1], load.at[0])
    loads = [
        pltpu.make_async_copy(off_hbm, off_ref, load.at[1]),
        pltpu.make_async_copy(cnt_hbm, cnt_ref, load.at[2]),
    ]
    tables = pltpu.make_async_copy(tab_hbm, tab_ref, load.at[0])
    pattern = pltpu.make_async_copy(pat_hbm, pat_ref, load.at[0])
    probes = [pltpu.make_async_copy(probe_hbm.at[mode_at(j)], probe_ref.at[j], load.at[3]) for j in range(modes)]
    all_probes = pltpu.make_async_copy(probe_hbm, probe_ref, load.at[3])

    barrier = pltpu.get_barrier_semaphore()

    def greet(to):
        pl.semaphore_signal(barrier, inc=1, device_id=to, device_id_type=MESH)

    pl.when(has_far)(lambda: greet({"row": far_row}))
    greet({"row": near})
    greet(mate)
    for copy in [obj_load] + probes + loads + [tables, pattern]:
        copy.start()
    with mark("w_barrier"):
        pl.semaphore_wait(barrier, 2 + has_far.astype(jnp.int32))

    rounds = tells(rows)

    def sides(r):
        return (me - rounds[r], me - rounds[r] >= 0), (me + rounds[r], me + rounds[r] < rows)

    def tell(r):
        for row, there in sides(r):

            @pl.when(there)
            def _():
                pl.semaphore_signal(news.at[r], inc=1, device_id={"row": row}, device_id_type=MESH)

    def hear(r):
        (_, above), (_, below) = sides(r)
        pl.semaphore_wait(news.at[r], above.astype(jnp.int32) + below.astype(jnp.int32))

    def remote(src, dst, send, recv, to):
        return pltpu.make_async_remote_copy(
            src_ref=src, dst_ref=dst, send_sem=send, recv_sem=recv, device_id=to, device_id_type=MESH
        )

    seen = 2 * col
    mine = 2 - 2 * col
    unit = 2 * n // sum(STRIPS)
    starts = [unit * sum(STRIPS[:i]) for i in range(len(STRIPS) + 1)]
    strips = [pl.ds(starts[i], starts[i + 1] - starts[i]) for i in range(len(STRIPS))]
    to_mate = remote(obj_hbm, frame.at[1, seen], sent.at[0], hm_recv.at[0], mate)

    def to_near(i, at=None):
        at = strips[i] if at is None else at
        return remote(obj_hbm.at[at], frame.at[far_at, 1, at], sent.at[0], n_recv.at[i], {"row": near})

    def to_far(i, at=None):
        at = strips[i] if at is None else at
        return remote(obj_hbm.at[at], frame.at[near_at, 1, at], sent_on.at[0], f_recv.at[i], {"row": far_row})

    def pass_on(i, at=None):
        at = strips[i] if at is None else at
        return remote(
            frame.at[near_at, 1, at], frame.at[far_at, 1, at], sent_on.at[0], f_recv.at[i], {"row": behind}
        )

    def relay(block, kind, at):
        return remote(
            frame.at[block, 1, at], frame.at[block, seen, at], (sent, sent_far)[kind].at[0], r_recv.at[kind], mate
        )

    whole = pl.ds(0, 2 * n)
    last = len(STRIPS)
    for i in range(last):
        to_near(i).start()
    for i in range(last):
        pl.when(direct)(to_far(i).start)
    to_mate.start()

    zero = jnp.zeros((2 * n, n), F32)
    for j in range(3):
        frame[j, seen] = zero

    @pl.when(jnp.logical_not(has_far))
    def _():
        frame[far_at, 1] = zero
        frame[far_at, mine] = zero

    @pl.when(jnp.logical_not(direct))
    def _():
        gfar[...] = zero

    with mark("w_load"):
        all_probes.wait()
    power = jnp.zeros((n, n), F32)
    for k in range(modes):
        power = power + (probe_ref[k, 0] * probe_ref[k, 0] + probe_ref[k, 1] * probe_ref[k, 1])
    weight = jnp.max(power) + epsilon

    with mark("w_halo"):
        def far_strip(i):
            @pl.when(has_far)
            def _():
                to_far(i).wait_recv()
                relay(far_at, 1, strips[i]).start()

        def near_strip(i):
            to_near(i).wait_recv()
            pl.when(passes)(pass_on(i).start)
            relay(near_at, 0, strips[i]).start()

        for i in range(last):
            near_strip(i)
        for i in range(last):
            far_strip(i)

    tell(0)
    for copy in loads:
        copy.wait()
    loaded = tally.at[pl.ds(0, 2 * n + pat_ref.shape[2] * n + 8 * n)]
    pltpu.make_async_copy(loaded, loaded, load.at[0]).wait()
    to_mate.wait_recv()
    with mark("w_relay"):
        relay(near_at, 0, whole).wait_recv()
        pl.when(has_far)(relay(far_at, 1, whole).wait_recv)

    r_hi, r_lo, l_hi, l_lo = (tab_ref.at[t] for t in range(4))
    row_id = lax.broadcasted_iota(jnp.int32, (n, n), 0)
    lane_id = lax.broadcasted_iota(jnp.int32, (n, n), 1)

    def place(s):
        oy, ox = off_ref[0, 0, s, 0], off_ref[0, 0, s, 1]
        by, bx = oy // n, ox // n
        return by, bx, oy - by * n, ox - bx * n

    for s in range(slots):
        by, bx, sy, sx = place(s)
        by2, bx2 = jnp.minimum(by + 1, 2), jnp.minimum(bx + 1, 2)
        for q in range(2):
            half = slice(q * n, (q + 1) * n)
            upper = jnp.where(lane_id >= sx, frame[by, bx, half], frame[by, bx2, half])
            lower = jnp.where(lane_id >= sx, frame[by2, bx, half], frame[by2, bx2, half])
            packed = jnp.where(row_id >= sy, upper, lower)
            packed = pltpu.roll(packed, lax.rem(n - sy, n), 0)
            win[s, q] = pltpu.roll(packed, lax.rem(n - sx, n), 1)
    for s in range(slots):
        for k in range(modes):
            wr, wi = win[s, 0], win[s, 1]
            pr, pi = probe_ref[k, 0], probe_ref[k, 1]
            for q, value in enumerate((pr * wr - pi * wi, pr * wi + pi * wr)):
                hi, lo = split(value)
                xh[s, k * n : (k + 1) * n, q * n : (q + 1) * n] = hi
                xl[s, k * n : (k + 1) * n, q * n : (q + 1) * n] = lo
    for s in range(slots):
        for k in range(modes):
            a_hi, a_lo = xh[s, k * n : (k + 1) * n, :], xl[s, k * n : (k + 1) * n, :]
            y = right3(a_hi, a_lo, r_hi[...], r_lo[...])
            for q in range(2):
                hi, lo = split(y[:, q * n : (q + 1) * n])
                yh[s, q * n : (q + 1) * n, k * n : (k + 1) * n] = hi
                yl[s, q * n : (q + 1) * n, k * n : (k + 1) * n] = lo
    for s in range(slots):
        for p in range(modes // 2):
            cols = slice(2 * p * n, 2 * (p + 1) * n)
            b_hi, b_lo = yh[s, :, cols], yl[s, :, cols]
            far[s, :, cols] = left3(l_hi[...], l_lo[...], b_hi, b_lo)
    for s in range(slots):
        level = jnp.zeros((n, n), F32)
        for k in range(modes):
            cols = slice(k * n, (k + 1) * n)
            level = level + far[s, :n, cols] * far[s, :n, cols] + far[s, n:, cols] * far[s, n:, cols]
        live = (s < cnt_ref[0, 0]).astype(F32)
        misfit = live * (level - pat_ref[0, 0, s])
        for k in range(modes):
            for q in range(2):
                spot = (s, slice(q * n, (q + 1) * n), slice(k * n, (k + 1) * n))
                hi, lo = split(misfit * far[spot])
                yh[spot] = hi
                yl[spot] = lo

    def to_partner(p):
        return remote(term.at[p], tpart.at[p], sent.at[0], t_recv.at[p], mate)

    def rows_of(owner, c):
        return pl.ds(pl.multiple_of(owner * slab + c * chunk, 8), chunk)

    def scatter(p, c, hop):
        return remote(
            acc.at[p, rows_of(hop_to(seat, hop), c)], pieces.at[p, c, hop - 1],
            sent.at[0], rs_recv.at[p, c], {"row": hop_to(me, hop)},
        )

    hops = list(range(1, group))
    for b in range(modes // 2):
        cols = slice(2 * b * n, 2 * (b + 1) * n)
        for s in range(slots):
            b_hi, b_lo = yh[s, :, cols], yl[s, :, cols]
            v = left3(r_hi[...], r_lo[...], b_hi, b_lo)
            for m in range(2):
                for q in range(2):
                    hi, lo = split(v[q * n : (q + 1) * n, m * n : (m + 1) * n])
                    vh[s, m * n : (m + 1) * n, q * n : (q + 1) * n] = hi
                    vl[s, m * n : (m + 1) * n, q * n : (q + 1) * n] = lo
        for m in range(2):
            k = 2 * b + m
            for s in range(slots):
                a_hi, a_lo = vh[s, m * n : (m + 1) * n, :], vl[s, m * n : (m + 1) * n, :]
                back = right3(a_hi, a_lo, l_hi[...], l_lo[...])
                br, bi = back[:, :n], back[:, n:]
                pr, pi = probe_ref[k, 0], probe_ref[k, 1]
                gr, gi = pr * br + pi * bi, pr * bi - pi * br
                wr, wi = win[s, 0], win[s, 1]
                tr, ti = wr * br + wi * bi, wr * bi - wi * br
                if k == 0:
                    gacc[s, 0], gacc[s, 1] = gr, gi
                else:
                    gacc[s, 0], gacc[s, 1] = gacc[s, 0] + gr, gacc[s, 1] + gi
                if s == 0:
                    term[k, :n], term[k, n:] = tr, ti
                else:
                    term[k, :n], term[k, n:] = term[k, :n] + tr, term[k, n:] + ti
            if k < pairs:
                to_partner(k).start()
            else:
                p = k - pairs
                with mark("w_partner"):
                    to_partner(p).wait_recv()
                if p == 0:
                    for r in range(len(rounds)):
                        hear(r)
                        if r + 1 < len(rounds):
                            tell(r + 1)
                acc[p] = term[k] + tpart[p]
                for c in range(CUTS):
                    for hop in hops[::-1]:
                        scatter(p, c, hop).start()

    def across(j):
        return remote(gpar.at[j], grecv.at[j], sent.at[0], g_recv.at[j], mate)

    for q in range(2):
        own = [jnp.zeros((n, n), F32)] * 3
        par = [jnp.zeros((n, n), F32)] * 3
        for s in range(slots):
            by, bx, sy, sx = place(s)
            g = pltpu.roll(pltpu.roll(gacc[s, q], sy, 0), sx, 1)
            low_x, low_y = (lane_id >= sx).astype(F32), (row_id >= sy).astype(F32)

            def side_of(block, at, low):
                return (block == at).astype(F32) * low + (block == at + 1).astype(F32) * (1.0 - low)

            g_own, g_par = g * side_of(1, bx, low_x), g * side_of(mine, bx, low_x)
            for j in range(3):
                mask = side_of(j, by, low_y)
                own[j] = own[j] + g_own * mask
                par[j] = par[j] + g_par * mask
        for j in range(3):
            gown[j, q * n : (q + 1) * n] = own[j]
            gpar[j, q * n : (q + 1) * n] = par[j]
    edge_far = remote(gown.at[far_at], gfar, sent_far.at[0], e_recv.at[0], {"row": far_row})
    edge_via = remote(gown.at[far_at], gvia, sent_far.at[0], e_recv.at[2], {"row": beyond})
    edge_near = remote(gown.at[near_at], gnear, sent.at[0], e_recv.at[1], {"row": near})
    for j in (far_at, near_at, 1):
        across(j).start()
    with mark("w_across"):
        for j in (far_at, near_at):
            across(j).wait_recv()
            gown[j] = gown[j] + grecv[j]
        pl.when(passed)(edge_via.start)

    chunks = [(p, c) for p in range(pairs) for c in range(CUTS)]

    def exchange(r, p, c):
        return remote(
            part.at[p, c, r], swapped.at[p, c, r], sent.at[0], x_recv.at[p, c, r], {"row": flip(me, ways[r])}
        )

    def gather(p, c, hop):
        here = fin.at[p, rows_of(seat, c)]
        return remote(here, here, sent.at[0], ag_recv.at[p, c], {"row": hop_to(me, hop)})

    def gather_other(p, c, hop):
        return remote(
            fin.at[p, rows_of(seat, c)], fin_other.at[p, rows_of(seat, c)], sent.at[0], o_recv.at[p],
            {"row": hop_to(me, hop), "col": 1 - col},
        )

    def share(p, c, hop):
        at = rows_of(hop_to(seat, hop), c)
        return remote(fin.at[p, at], fin_other.at[p, at], sent.at[0], o_recv.at[p], mate)

    def settle(r, p, c, total):
        if r < len(ways):
            part[p, c, r] = total
            exchange(r, p, c).start()
        else:
            fin[p, rows_of(seat, c)] = total
            for hop in hops:
                gather(p, c, hop).start()
                if (p, c) == chunks[-1]:
                    gather_other(p, c, hop).start()
            share(p, c, 0).start()

    def all_of(ref, recv):
        return remote(ref, ref, sent.at[0], recv, mate)

    for p, c in chunks:
        total = acc[p, rows_of(seat, c)]
        with mark("w_rs"):
            all_of(pieces.at[p, c], rs_recv.at[p, c]).wait_recv()
        for hop in hops:
            total = total + pieces[p, c, hop - 1]
        settle(0, p, c, total)
        if (p, c) == chunks[0]:
            pl.when(col == 0)(edge_near.start)
    pl.when(direct)(edge_far.start)

    with mark("w_via"):

        @pl.when(passes)
        def _():
            edge_via.wait_recv()
            gown[near_at] = gown[near_at] + gvia[...]

        pl.when(col == 1)(edge_near.start)
    for r in range(len(ways)):
        for p, c in chunks:
            with mark("w_xc"):
                exchange(r, p, c).wait_recv()
            settle(r + 1, p, c, part[p, c, r] + swapped[p, c, r])

    for p, c in chunks:
        with mark("w_ag"):
            all_of(pieces.at[p, c], ag_recv.at[p, c]).wait_recv()
        for hop in hops:
            if (p, c) != chunks[-1]:
                share(p, c, hop).start()
    for p in range(pairs):
        for q in range(2):
            half = slice(q * n, (q + 1) * n)
            probe_out[2 * p + col, q] = probe_ref[pairs + p, q] - (probe_rate / tiles) * fin[p, half]
    with mark("w_edge"):
        across(1).wait_recv()
        edge_near.wait_recv()
        pl.when(direct)(edge_far.wait_recv)
    for q in range(2):
        half = slice(q * n, (q + 1) * n)
        grad = gown[1, half] + grecv[1, half] + gnear[half] + gfar[half]
        obj_out[half] = frame[1, 1, half] - object_rate * grad / weight

    for p in range(pairs):
        with mark("w_share"):
            all_of(fin_other.at[p], o_recv.at[p]).wait_recv()
        for q in range(2):
            half = slice(q * n, (q + 1) * n)
            probe_out[2 * p + 1 - col, q] = probe_ref[p, q] - (probe_rate / tiles) * fin_other[p, half]

    with mark("w_sends"):
        def drain(count, sem):
            here = tally.at[pl.ds(0, count)]
            remote(here, here, sem.at[0], hm_recv.at[0], mate).wait_send()

        drain(tally.shape[0], sent)
        pl.when(has_far)(lambda: drain(4 * n, sent_far))
        pl.when(jnp.logical_or(direct, passes))(lambda: drain(2 * n, sent_on))


def finish(obj_ref, probe_ref, obj_out, probe_out, sem):
    copies = [pltpu.make_async_copy(obj_ref, obj_out, sem.at[0])]
    for k in range(probe_ref.shape[0]):
        copies.append(pltpu.make_async_copy(probe_ref.at[k], probe_out.at[k], sem.at[k + 1]))
    for copy in copies:
        copy.start()
    for copy in copies:
        copy.wait()


def body(rows, object_field, probe, patterns, offsets, counts):
    modes, _, n, _ = probe.shape
    slots = patterns.shape[2]
    pairs = modes // 2
    assert rows > 1
    group, ways = plan(rows)
    block = object_field.reshape(2 * n, n)
    rounds = max(1, len(ways))
    chunk = 2 * n // group // CUTS
    rows_sent = 2 * n * (4 + pairs + 3 + pairs) + pairs * CUTS * chunk * (2 * (group - 1) + len(ways))
    tables = jnp.asarray(dft_tables(n))
    vmem = pl.BlockSpec(memory_space=pltpu.VMEM)
    hbm = pl.BlockSpec(memory_space=pltpu.HBM)
    dma = pltpu.SemaphoreType.DMA
    wide, tall = (slots, 2 * n, modes * n), (slots, modes * n, 2 * n)
    outs = (
        jax.ShapeDtypeStruct(block.shape, F32),
        jax.ShapeDtypeStruct(probe.shape, F32),
    )
    results = pl.pallas_call(
        functools.partial(kernel, rows, modes, slots, n),
        out_shape=outs,
        in_specs=[hbm] * 6,
        out_specs=(vmem, vmem),
        scratch_shapes=[
            pltpu.SMEM(offsets.shape, jnp.int32),
            pltpu.SMEM(counts.shape, jnp.int32),
            pltpu.VMEM(probe.shape, F32),
            pltpu.VMEM(patterns.shape, F32),
            pltpu.VMEM(tables.shape, BF16),
            pltpu.VMEM((3, 3, 2 * n, n), F32),
            pltpu.VMEM(tall, BF16),
            pltpu.VMEM(tall, BF16),
            pltpu.VMEM(wide, BF16),
            pltpu.VMEM(wide, BF16),
            pltpu.VMEM(wide, F32),
            pltpu.VMEM((slots, 2 * n, 2 * n), BF16),
            pltpu.VMEM((slots, 2 * n, 2 * n), BF16),
            pltpu.VMEM((slots, 2, n, n), F32),
            pltpu.VMEM((slots, 2, n, n), F32),
            pltpu.VMEM((3, 2 * n, n), F32),
            pltpu.VMEM((3, 2 * n, n), F32),
            pltpu.VMEM((3, 2 * n, n), F32),
            pltpu.VMEM((2 * n, n), F32),
            pltpu.VMEM((2 * n, n), F32),
            pltpu.VMEM((2 * n, n), F32),
            pltpu.VMEM((rows_sent, n), F32),
            pltpu.VMEM((modes, 2 * n, n), F32),
            pltpu.VMEM((pairs, 2 * n, n), F32),
            pltpu.VMEM((pairs, 2 * n, n), F32),
            pltpu.VMEM((pairs, CUTS, group - 1, chunk, n), F32),
            pltpu.VMEM((pairs, CUTS, rounds, chunk, n), F32),
            pltpu.VMEM((pairs, CUTS, rounds, chunk, n), F32),
            pltpu.VMEM((pairs, 2 * n, n), F32),
            pltpu.VMEM((pairs, 2 * n, n), F32),
            dma((4,)), dma((1,)), dma((1,)), dma((1,)),
            dma((1,)), dma((len(STRIPS),)), dma((len(STRIPS),)), dma((2,)), dma((3,)),
            dma((3,)), dma((pairs,)), dma((pairs, CUTS)), dma((pairs, CUTS, rounds)),
            dma((pairs, CUTS)), dma((pairs,)),
            pltpu.SemaphoreType.REGULAR((len(tells(rows)),)),
        ],
        compiler_params=pltpu.CompilerParams(
            collective_id=0, has_side_effects=True, vmem_limit_bytes=24 << 20
        ),
    )(*[pltpu.with_memory_space_constraint(x, pltpu.HBM) for x in (offsets,)], counts, *[pltpu.with_memory_space_constraint(x, pltpu.HBM) for x in (block, probe, patterns, tables)])
    new_block, new_probe = pl.pallas_call(
        finish,
        out_shape=outs,
        in_specs=[vmem] * 2,
        out_specs=(hbm, hbm),
        scratch_shapes=[dma((1 + modes,))],
        compiler_params=pltpu.CompilerParams(vmem_limit_bytes=4 << 20),
    )(*results)
    return new_block.reshape(object_field.shape), new_probe


def solution(mesh):
    placed = (
        P(None, ("tilt", "row"), "col"),
        P("tilt", None, None, None),
        P(("tilt", "row"), "col", None, None, None),
        P(("tilt", "row"), "col", None, None),
        P(("tilt", "row"), "col"),
    )
    return jax.shard_map(
        functools.partial(body, mesh.shape["row"]),
        mesh=mesh,
        in_specs=placed,
        out_specs=(P(None, ("tilt", "row"), "col"), P("tilt", None, None, None)),
        check_vma=False,
    )
```

```python
import contextlib
import functools

import jax
import jax.numpy as jnp
import numpy as np
from jax import lax
from jax.experimental import pallas as pl
from jax.experimental.pallas import tpu as pltpu
from jax.sharding import PartitionSpec as P

MESH = pl.DeviceIdType.MESH
F32 = jnp.float32
BF16 = jnp.bfloat16

object_rate = 1.0
probe_rate = 1.0
epsilon = 1e-06


def mark(name):
    return contextlib.nullcontext()


def split_table(table):
    high = table.astype(jnp.bfloat16)
    low = (table - high.astype(np.float64)).astype(jnp.bfloat16)
    return high, low


def dft_tables(length):
    counter = np.arange(length)
    product = counter[:, None] * counter[None, :] % length
    angle = -2.0 * np.pi / length * product
    c, s = np.cos(angle) / np.sqrt(length), np.sin(angle) / np.sqrt(length)
    right = np.block([[c, s], [-s, c]])
    left = right.T
    return np.stack([*split_table(right), *split_table(left)])


def split(x):
    high = x.astype(BF16)
    return high, (x - high.astype(F32)).astype(BF16)


def dot(a, b):
    return jnp.dot(a, b, preferred_element_type=F32)


def right3(a_hi, a_lo, hi, lo):
    m = a_hi.shape[0]
    both = dot(jnp.concatenate([a_hi, a_lo], 0), hi)
    return both[:m] + both[m:] + dot(a_hi, lo)


def left3(hi, lo, b_hi, b_lo):
    m = hi.shape[0]
    both = dot(jnp.concatenate([hi, lo], 0), b_hi)
    return both[:m] + both[m:] + dot(hi, b_lo)


def plan(rows):
    assert rows & (rows - 1) == 0
    group = min(4, rows)
    ways = []
    while group << len(ways) < rows:
        ways.append(group << len(ways))
    return group, ways


def tells(rows):
    distances = [2]
    while 4 * distances[-1] < rows:
        distances.append(2 * distances[-1])
    return distances


CUTS = 2
STRIPS = (3, 3, 2)


def kernel(
    rows, modes, slots, width,
    off_hbm, cnt_hbm, obj_hbm, probe_hbm, pat_hbm, tab_hbm,
    obj_out, probe_out,
    off_ref, cnt_ref, probe_ref, pat_ref, tab_ref,
    frame, xh, xl, yh, yl, far, vh, vl, win, gacc,
    gown, gpar, grecv, gnear, gfar, gvia, tally, term, tpart, acc, pieces, part, swapped, fin, fin_other,
    load, sent, sent_far, sent_on, n_recv, f_recv, r_recv, g_recv,
    e_recv, t_recv, rs_recv, x_recv, ag_recv, o_recv, news,
):
    me = lax.axis_index("row")
    col = lax.axis_index("col")
    n = width
    tiles = rows * 2
    pairs = modes // 2
    group, ways = plan(rows)
    slab = 2 * n // group
    chunk = slab // CUTS
    mate = {"col": 1 - col}
    odd = lax.rem(me, 2)
    near_at, far_at = 2 - 2 * odd, 2 * odd
    near, far_row, beyond, behind = me + 1 - 2 * odd, me - 1 + 2 * odd, me - 2 + 4 * odd, me + 2 - 4 * odd
    has_far = jnp.logical_and(far_row >= 0, far_row < rows)
    direct = jnp.logical_and(has_far, col == 0)
    passes = jnp.logical_and(jnp.logical_and(behind >= 0, behind < rows), col == 1)
    passed = jnp.logical_and(has_far, col == 1)
    seat = lax.rem(me, group)

    def flip(index, bit):
        return jnp.where(lax.rem(index // bit, 2) == 0, index + bit, index - bit)

    def hop_to(index, hop):
        for b in range(hop.bit_length()):
            if hop >> b & 1:
                index = flip(index, 1 << b)
        return index

    def mode_at(spot):
        return 2 * spot + 1 - col if spot < pairs else 2 * (spot - pairs) + col

    obj_load = pltpu.make_async_copy(obj_hbm, frame.at[1, 1], load.at[0])
    loads = [
        pltpu.make_async_copy(off_hbm, off_ref, load.at[1]),
        pltpu.make_async_copy(cnt_hbm, cnt_ref, load.at[2]),
    ]
    tables = pltpu.make_async_copy(tab_hbm, tab_ref, load.at[0])
    pattern = pltpu.make_async_copy(pat_hbm, pat_ref, load.at[0])
    probes = [pltpu.make_async_copy(probe_hbm.at[mode_at(j)], probe_ref.at[j], load.at[3]) for j in range(modes)]
    all_probes = pltpu.make_async_copy(probe_hbm, probe_ref, load.at[3])

    barrier = pltpu.get_barrier_semaphore()

    def greet(to):
        pl.semaphore_signal(barrier, inc=1, device_id=to, device_id_type=MESH)

    pl.when(has_far)(lambda: greet({"row": far_row}))
    greet({"row": near})
    greet(mate)
    for copy in [obj_load] + probes + loads + [tables, pattern]:
        copy.start()
    with mark("w_barrier"):
        pl.semaphore_wait(barrier, 2 + has_far.astype(jnp.int32))

    rounds = tells(rows)

    def sides(r):
        return (me - rounds[r], me - rounds[r] >= 0), (me + rounds[r], me + rounds[r] < rows)

    def tell(r):
        for row, there in sides(r):

            @pl.when(there)
            def _():
                pl.semaphore_signal(news.at[r], inc=1, device_id={"row": row}, device_id_type=MESH)

    def hear(r):
        (_, above), (_, below) = sides(r)
        pl.semaphore_wait(news.at[r], above.astype(jnp.int32) + below.astype(jnp.int32))

    def remote(src, dst, send, recv, to):
        return pltpu.make_async_remote_copy(
            src_ref=src, dst_ref=dst, send_sem=send, recv_sem=recv, device_id=to, device_id_type=MESH
        )

    seen = 2 * col
    mine = 2 - 2 * col
    unit = 2 * n // sum(STRIPS)
    starts = [unit * sum(STRIPS[:i]) for i in range(len(STRIPS) + 1)]
    strips = [pl.ds(starts[i], starts[i + 1] - starts[i]) for i in range(len(STRIPS))]
    to_mate = remote(obj_hbm, frame.at[1, seen], sent.at[0], r_recv.at[0], mate)

    def to_near(i, at=None):
        at = strips[i] if at is None else at
        return remote(obj_hbm.at[at], frame.at[far_at, 1, at], sent.at[0], n_recv.at[i], {"row": near})

    def to_far(i, at=None):
        at = strips[i] if at is None else at
        return remote(obj_hbm.at[at], frame.at[near_at, 1, at], sent_on.at[0], f_recv.at[i], {"row": far_row})

    def pass_on(i, at=None):
        at = strips[i] if at is None else at
        return remote(
            frame.at[near_at, 1, at], frame.at[far_at, 1, at], sent_on.at[0], f_recv.at[i], {"row": behind}
        )

    def relay(block, kind, at):
        return remote(
            frame.at[block, 1, at], frame.at[block, seen, at], (sent, sent_far)[kind].at[0], r_recv.at[kind], mate
        )

    whole = pl.ds(0, 2 * n)
    last = len(STRIPS)
    for i in range(last):
        to_near(i).start()
    for i in range(last):
        pl.when(direct)(to_far(i).start)
    to_mate.start()

    zero = jnp.zeros((2 * n, n), F32)
    for j in range(3):
        frame[j, seen] = zero

    @pl.when(jnp.logical_not(has_far))
    def _():
        frame[far_at, 1] = zero
        frame[far_at, mine] = zero

    @pl.when(jnp.logical_not(direct))
    def _():
        gfar[...] = zero

    with mark("w_load"):
        all_probes.wait()
    power = jnp.zeros((n, n), F32)
    for k in range(modes):
        power = power + (probe_ref[k, 0] * probe_ref[k, 0] + probe_ref[k, 1] * probe_ref[k, 1])
    weight = jnp.max(power) + epsilon

    with mark("w_halo"):
        def far_strip(i):
            @pl.when(has_far)
            def _():
                to_far(i).wait_recv()
                relay(far_at, 1, strips[i]).start()

        def near_strip(i):
            to_near(i).wait_recv()
            pl.when(passes)(pass_on(i).start)
            relay(near_at, 0, strips[i]).start()

        for i in range(last):
            near_strip(i)
        for i in range(last):
            far_strip(i)

    tell(0)
    for copy in loads:
        copy.wait()
    loaded = tally.at[pl.ds(0, 2 * n + pat_ref.shape[2] * n + 8 * n)]
    pltpu.make_async_copy(loaded, loaded, load.at[0]).wait()
    with mark("w_relay"):
        both = tally.at[pl.ds(0, 4 * n)]
        remote(both, both, sent.at[0], r_recv.at[0], mate).wait_recv()
        pl.when(has_far)(relay(far_at, 1, whole).wait_recv)

    r_hi, r_lo, l_hi, l_lo = (tab_ref.at[t] for t in range(4))
    row_id = lax.broadcasted_iota(jnp.int32, (n, n), 0)
    lane_id = lax.broadcasted_iota(jnp.int32, (n, n), 1)

    def place(s):
        oy, ox = off_ref[0, 0, s, 0], off_ref[0, 0, s, 1]
        by, bx = oy // n, ox // n
        return by, bx, oy - by * n, ox - bx * n

    for s in range(slots):
        by, bx, sy, sx = place(s)
        by2, bx2 = jnp.minimum(by + 1, 2), jnp.minimum(bx + 1, 2)
        for q in range(2):
            half = slice(q * n, (q + 1) * n)
            upper = jnp.where(lane_id >= sx, frame[by, bx, half], frame[by, bx2, half])
            lower = jnp.where(lane_id >= sx, frame[by2, bx, half], frame[by2, bx2, half])
            packed = jnp.where(row_id >= sy, upper, lower)
            packed = pltpu.roll(packed, lax.rem(n - sy, n), 0)
            win[s, q] = pltpu.roll(packed, lax.rem(n - sx, n), 1)
    for s in range(slots):
        for k in range(modes):
            wr, wi = win[s, 0], win[s, 1]
            pr, pi = probe_ref[k, 0], probe_ref[k, 1]
            for q, value in enumerate((pr * wr - pi * wi, pr * wi + pi * wr)):
                hi, lo = split(value)
                xh[s, k * n : (k + 1) * n, q * n : (q + 1) * n] = hi
                xl[s, k * n : (k + 1) * n, q * n : (q + 1) * n] = lo
    for s in range(slots):
        for k in range(modes):
            a_hi, a_lo = xh[s, k * n : (k + 1) * n, :], xl[s, k * n : (k + 1) * n, :]
            y = right3(a_hi, a_lo, r_hi[...], r_lo[...])
            for q in range(2):
                hi, lo = split(y[:, q * n : (q + 1) * n])
                yh[s, q * n : (q + 1) * n, k * n : (k + 1) * n] = hi
                yl[s, q * n : (q + 1) * n, k * n : (k + 1) * n] = lo
    for s in range(slots):
        for p in range(modes // 2):
            cols = slice(2 * p * n, 2 * (p + 1) * n)
            b_hi, b_lo = yh[s, :, cols], yl[s, :, cols]
            far[s, :, cols] = left3(l_hi[...], l_lo[...], b_hi, b_lo)
    for s in range(slots):
        level = jnp.zeros((n, n), F32)
        for k in range(modes):
            cols = slice(k * n, (k + 1) * n)
            level = level + far[s, :n, cols] * far[s, :n, cols] + far[s, n:, cols] * far[s, n:, cols]
        live = (s < cnt_ref[0, 0]).astype(F32)
        misfit = live * (level - pat_ref[0, 0, s])
        for k in range(modes):
            for q in range(2):
                spot = (s, slice(q * n, (q + 1) * n), slice(k * n, (k + 1) * n))
                hi, lo = split(misfit * far[spot])
                yh[spot] = hi
                yl[spot] = lo

    def to_partner(p):
        return remote(term.at[p], tpart.at[p], sent.at[0], t_recv.at[p], mate)

    def rows_of(owner, c):
        return pl.ds(pl.multiple_of(owner * slab + c * chunk, 8), chunk)

    def scatter(p, c, hop):
        return remote(
            acc.at[p, rows_of(hop_to(seat, hop), c)], pieces.at[p, c, hop - 1],
            sent.at[0], rs_recv.at[p, c], {"row": hop_to(me, hop)},
        )

    hops = list(range(1, group))
    for b in range(modes // 2):
        cols = slice(2 * b * n, 2 * (b + 1) * n)
        for s in range(slots):
            b_hi, b_lo = yh[s, :, cols], yl[s, :, cols]
            v = left3(r_hi[...], r_lo[...], b_hi, b_lo)
            for m in range(2):
                for q in range(2):
                    hi, lo = split(v[q * n : (q + 1) * n, m * n : (m + 1) * n])
                    vh[s, m * n : (m + 1) * n, q * n : (q + 1) * n] = hi
                    vl[s, m * n : (m + 1) * n, q * n : (q + 1) * n] = lo
        for m in range(2):
            k = 2 * b + m
            for s in range(slots):
                a_hi, a_lo = vh[s, m * n : (m + 1) * n, :], vl[s, m * n : (m + 1) * n, :]
                back = right3(a_hi, a_lo, l_hi[...], l_lo[...])
                br, bi = back[:, :n], back[:, n:]
                pr, pi = probe_ref[k, 0], probe_ref[k, 1]
                gr, gi = pr * br + pi * bi, pr * bi - pi * br
                wr, wi = win[s, 0], win[s, 1]
                tr, ti = wr * br + wi * bi, wr * bi - wi * br
                if k == 0:
                    gacc[s, 0], gacc[s, 1] = gr, gi
                else:
                    gacc[s, 0], gacc[s, 1] = gacc[s, 0] + gr, gacc[s, 1] + gi
                if s == 0:
                    term[k, :n], term[k, n:] = tr, ti
                else:
                    term[k, :n], term[k, n:] = term[k, :n] + tr, term[k, n:] + ti
            if k < pairs:
                to_partner(k).start()
            else:
                p = k - pairs
                with mark("w_partner"):
                    to_partner(p).wait_recv()
                if p == 0:
                    for r in range(len(rounds)):
                        hear(r)
                        if r + 1 < len(rounds):
                            tell(r + 1)
                acc[p] = term[k] + tpart[p]
                for c in range(CUTS):
                    for hop in hops[::-1]:
                        scatter(p, c, hop).start()

    def across(j):
        return remote(gpar.at[j], grecv.at[j], sent.at[0], g_recv.at[j], mate)

    for q in range(2):
        own = [jnp.zeros((n, n), F32)] * 3
        par = [jnp.zeros((n, n), F32)] * 3
        for s in range(slots):
            by, bx, sy, sx = place(s)
            g = pltpu.roll(pltpu.roll(gacc[s, q], sy, 0), sx, 1)
            low_x, low_y = (lane_id >= sx).astype(F32), (row_id >= sy).astype(F32)

            def side_of(block, at, low):
                return (block == at).astype(F32) * low + (block == at + 1).astype(F32) * (1.0 - low)

            g_own, g_par = g * side_of(1, bx, low_x), g * side_of(mine, bx, low_x)
            for j in range(3):
                mask = side_of(j, by, low_y)
                own[j] = own[j] + g_own * mask
                par[j] = par[j] + g_par * mask
        for j in range(3):
            gown[j, q * n : (q + 1) * n] = own[j]
            gpar[j, q * n : (q + 1) * n] = par[j]
    edge_far = remote(gown.at[far_at], gfar, sent_far.at[0], e_recv.at[0], {"row": far_row})
    edge_via = remote(gown.at[far_at], gvia, sent_far.at[0], e_recv.at[2], {"row": beyond})
    edge_near = remote(gown.at[near_at], gnear, sent.at[0], e_recv.at[1], {"row": near})
    for j in (far_at, near_at, 1):
        across(j).start()
    with mark("w_across"):
        for j in (far_at, near_at):
            across(j).wait_recv()
            gown[j] = gown[j] + grecv[j]
        pl.when(passed)(edge_via.start)

    chunks = [(p, c) for p in range(pairs) for c in range(CUTS)]

    def exchange(r, p, c):
        return remote(
            part.at[p, c, r], swapped.at[p, c, r], sent.at[0], x_recv.at[p, c, r], {"row": flip(me, ways[r])}
        )

    def gather(p, c, hop):
        here = fin.at[p, rows_of(seat, c)]
        return remote(here, here, sent.at[0], ag_recv.at[p, c], {"row": hop_to(me, hop)})

    def gather_other(p, c, hop):
        return remote(
            fin.at[p, rows_of(seat, c)], fin_other.at[p, rows_of(seat, c)], sent.at[0], o_recv.at[p],
            {"row": hop_to(me, hop), "col": 1 - col},
        )

    def share(p, c, hop):
        at = rows_of(hop_to(seat, hop), c)
        return remote(fin.at[p, at], fin_other.at[p, at], sent.at[0], o_recv.at[p], mate)

    def settle(r, p, c, total):
        if r < len(ways):
            part[p, c, r] = total
            exchange(r, p, c).start()
        else:
            fin[p, rows_of(seat, c)] = total
            for hop in hops:
                gather(p, c, hop).start()
                if (p, c) == chunks[-1]:
                    gather_other(p, c, hop).start()
            share(p, c, 0).start()

    def all_of(ref, recv):
        return remote(ref, ref, sent.at[0], recv, mate)

    for p, c in chunks:
        total = acc[p, rows_of(seat, c)]
        with mark("w_rs"):
            all_of(pieces.at[p, c], rs_recv.at[p, c]).wait_recv()
        for hop in hops:
            total = total + pieces[p, c, hop - 1]
        settle(0, p, c, total)
        if (p, c) == chunks[0]:
            pl.when(col == 0)(edge_near.start)
    pl.when(direct)(edge_far.start)

    with mark("w_via"):

        @pl.when(passes)
        def _():
            edge_via.wait_recv()
            gown[near_at] = gown[near_at] + gvia[...]

        pl.when(col == 1)(edge_near.start)
    for r in range(len(ways)):
        for p, c in chunks:
            with mark("w_xc"):
                exchange(r, p, c).wait_recv()
            settle(r + 1, p, c, part[p, c, r] + swapped[p, c, r])

    for p, c in chunks:
        with mark("w_ag"):
            all_of(pieces.at[p, c], ag_recv.at[p, c]).wait_recv()
        for hop in hops:
            if (p, c) != chunks[-1]:
                share(p, c, hop).start()
    for p in range(pairs):
        for q in range(2):
            half = slice(q * n, (q + 1) * n)
            probe_out[2 * p + col, q] = probe_ref[pairs + p, q] - (probe_rate / tiles) * fin[p, half]
    with mark("w_edge"):
        across(1).wait_recv()
        edge_near.wait_recv()
        pl.when(direct)(edge_far.wait_recv)
    for q in range(2):
        half = slice(q * n, (q + 1) * n)
        grad = gown[1, half] + grecv[1, half] + gnear[half] + gfar[half]
        obj_out[half] = frame[1, 1, half] - object_rate * grad / weight

    for p in range(pairs):
        with mark("w_share"):
            all_of(fin_other.at[p], o_recv.at[p]).wait_recv()
        for q in range(2):
            half = slice(q * n, (q + 1) * n)
            probe_out[2 * p + 1 - col, q] = probe_ref[p, q] - (probe_rate / tiles) * fin_other[p, half]

    with mark("w_sends"):
        def drain(count, sem):
            here = tally.at[pl.ds(0, count)]
            remote(here, here, sem.at[0], r_recv.at[0], mate).wait_send()

        drain(tally.shape[0], sent)
        pl.when(has_far)(lambda: drain(4 * n, sent_far))
        pl.when(jnp.logical_or(direct, passes))(lambda: drain(2 * n, sent_on))


def finish(obj_ref, probe_ref, obj_out, probe_out, sem):
    copies = [pltpu.make_async_copy(obj_ref, obj_out, sem.at[0])]
    for k in range(probe_ref.shape[0]):
        copies.append(pltpu.make_async_copy(probe_ref.at[k], probe_out.at[k], sem.at[k + 1]))
    for copy in copies:
        copy.start()
    for copy in copies:
        copy.wait()


def body(rows, object_field, probe, patterns, offsets, counts):
    modes, _, n, _ = probe.shape
    slots = patterns.shape[2]
    pairs = modes // 2
    assert rows > 1
    group, ways = plan(rows)
    block = object_field.reshape(2 * n, n)
    rounds = max(1, len(ways))
    chunk = 2 * n // group // CUTS
    rows_sent = 2 * n * (4 + pairs + 3 + pairs) + pairs * CUTS * chunk * (2 * (group - 1) + len(ways))
    tables = jnp.asarray(dft_tables(n))
    vmem = pl.BlockSpec(memory_space=pltpu.VMEM)
    hbm = pl.BlockSpec(memory_space=pltpu.HBM)
    dma = pltpu.SemaphoreType.DMA
    wide, tall = (slots, 2 * n, modes * n), (slots, modes * n, 2 * n)
    outs = (
        jax.ShapeDtypeStruct(block.shape, F32),
        jax.ShapeDtypeStruct(probe.shape, F32),
    )
    results = pl.pallas_call(
        functools.partial(kernel, rows, modes, slots, n),
        out_shape=outs,
        in_specs=[hbm] * 6,
        out_specs=(vmem, vmem),
        scratch_shapes=[
            pltpu.SMEM(offsets.shape, jnp.int32),
            pltpu.SMEM(counts.shape, jnp.int32),
            pltpu.VMEM(probe.shape, F32),
            pltpu.VMEM(patterns.shape, F32),
            pltpu.VMEM(tables.shape, BF16),
            pltpu.VMEM((3, 3, 2 * n, n), F32),
            pltpu.VMEM(tall, BF16),
            pltpu.VMEM(tall, BF16),
            pltpu.VMEM(wide, BF16),
            pltpu.VMEM(wide, BF16),
            pltpu.VMEM(wide, F32),
            pltpu.VMEM((slots, 2 * n, 2 * n), BF16),
            pltpu.VMEM((slots, 2 * n, 2 * n), BF16),
            pltpu.VMEM((slots, 2, n, n), F32),
            pltpu.VMEM((slots, 2, n, n), F32),
            pltpu.VMEM((3, 2 * n, n), F32),
            pltpu.VMEM((3, 2 * n, n), F32),
            pltpu.VMEM((3, 2 * n, n), F32),
            pltpu.VMEM((2 * n, n), F32),
            pltpu.VMEM((2 * n, n), F32),
            pltpu.VMEM((2 * n, n), F32),
            pltpu.VMEM((rows_sent, n), F32),
            pltpu.VMEM((modes, 2 * n, n), F32),
            pltpu.VMEM((pairs, 2 * n, n), F32),
            pltpu.VMEM((pairs, 2 * n, n), F32),
            pltpu.VMEM((pairs, CUTS, group - 1, chunk, n), F32),
            pltpu.VMEM((pairs, CUTS, rounds, chunk, n), F32),
            pltpu.VMEM((pairs, CUTS, rounds, chunk, n), F32),
            pltpu.VMEM((pairs, 2 * n, n), F32),
            pltpu.VMEM((pairs, 2 * n, n), F32),
            dma((4,)), dma((1,)), dma((1,)), dma((1,)),
            dma((len(STRIPS),)), dma((len(STRIPS),)), dma((2,)), dma((3,)),
            dma((3,)), dma((pairs,)), dma((pairs, CUTS)), dma((pairs, CUTS, rounds)),
            dma((pairs, CUTS)), dma((pairs,)),
            pltpu.SemaphoreType.REGULAR((len(tells(rows)),)),
        ],
        compiler_params=pltpu.CompilerParams(
            collective_id=0, has_side_effects=True, vmem_limit_bytes=24 << 20
        ),
    )(*[pltpu.with_memory_space_constraint(x, pltpu.HBM) for x in (offsets,)], counts, *[pltpu.with_memory_space_constraint(x, pltpu.HBM) for x in (block, probe, patterns, tables)])
    new_block, new_probe = pl.pallas_call(
        finish,
        out_shape=outs,
        in_specs=[vmem] * 2,
        out_specs=(hbm, hbm),
        scratch_shapes=[dma((1 + modes,))],
        compiler_params=pltpu.CompilerParams(vmem_limit_bytes=4 << 20),
    )(*results)
    return new_block.reshape(object_field.shape), new_probe


def solution(mesh):
    placed = (
        P(None, ("tilt", "row"), "col"),
        P("tilt", None, None, None),
        P(("tilt", "row"), "col", None, None, None),
        P(("tilt", "row"), "col", None, None),
        P(("tilt", "row"), "col"),
    )
    return jax.shard_map(
        functools.partial(body, mesh.shape["row"]),
        mesh=mesh,
        in_specs=placed,
        out_specs=(P(None, ("tilt", "row"), "col"), P("tilt", None, None, None)),
        check_vma=False,
    )
```
